256 devices in a mesh: horiz: 32 (over x, y, core), lev: 8 (over z).
Axes of the slice: x: 4, y: 4, z: 8, core: 2. Of those that a mesh axis runs over, the one named last changes fastest.
Arguments:
- source_state: bfloat16 [5, 136, 131072], P(None, 'lev', 'horiz'), may hold values from -6 to 6
- intersection: int32 [160], P('horiz'), may hold values from 0 to 31, as said below
- index_map: int32 [160, 512], P('horiz'), may hold values from 0 to 4095
- blocks: bfloat16 [160, 512, 2048], P('horiz'), may hold values from -0.125 to 0.125
- bracket: int32 [127, 65536], P(None, ('horiz', 'lev')), may hold values from 0 to 134
- fraction: float32 [127, 65536], P(None, ('horiz', 'lev')), may hold values from 0 to 1
Outputs:
- target_state: bfloat16 [5, 127, 65536], P(None, None, ('horiz', 'lev'))
The draws below stay inside these ranges and needn't reach their ends.
Inputs may be any that keep to these rules, and one draw needn't show every extreme that they name: For every target group g, intersection[g * 5] to intersection[g * 5 + 4] are the groups g - 2 to g + 2 modulo 32, each once, in some order.
All inputs are finite; a program needn't handle non-finite values.
Results may differ from the reference program's by a relative error of at most 0.0049.
Values may be sent and summed in bfloat16 or wider, within the bound.
A program may use at most 64 MiB of HBM per device.

```python
import jax
import jax.numpy as jnp
from jax import lax

F = 5
LEVELS_OUT = 127
R = 2
SRC_DEV = 4096
P_SIZE = 512
TGT_DEV = 2048
K = 5
GROUPS = 32
LEVELS_IN = 136
SRC_CELLS = 131072
TGT_CELLS = 65536
BLOCKS = 160


def draw_intersection(key, part):
    subkeys = jax.random.split(key, GROUPS)
    orders = jax.vmap(lambda subkey: jax.random.permutation(subkey, K))(subkeys)
    group_ids = jnp.arange(GROUPS, dtype=jnp.int32)[:, None]
    return ((group_ids + orders.astype(jnp.int32) - R) % GROUPS).reshape(-1).astype(jnp.int32)


def plant(drawn, key, least, high):
    extent = drawn.shape
    spot = [jax.random.randint(jax.random.fold_in(key, axis), (), 0, extent[axis]) for axis in range(len(extent))]
    drawn = drawn.at[tuple(spot)].set(least)
    longest = extent.index(max(extent))
    spot[longest] = (spot[longest] + 1) % extent[longest]
    return drawn.at[tuple(spot)].set(high)


def block_levels(key, extent, shards, smallest, top_value):
    def one(dim, parts):
        heights = jax.random.uniform(jax.random.fold_in(jax.random.fold_in(key, 6), dim), (parts,), jnp.float32, smallest / len(shards), top_value / len(shards))
        return jnp.repeat(jnp.exp(heights), extent[dim] // parts).reshape((-1,) + (1,) * (len(extent) - dim - 1))

    loudness = one(*shards[0])
    for cut in shards[1:]:
        loudness = loudness * one(*cut)
    return loudness


def scatter_about(key, dims, deviation, limit, pieces=(), held_as=jnp.bfloat16):
    array = jax.random.normal(key, dims, jnp.float32) * deviation
    if len(pieces) > 0:
        array = block_levels(key, dims, pieces, -0.22, 0.18) * array
    return jnp.clip(array, min=-limit, max=limit).astype(held_as)


def setup_inputs(seed: int = 0) -> dict:
    key_of = jax.random.split(jax.random.key(seed), 7)
    source_state = scatter_about(key_of[0], (F, LEVELS_IN, SRC_CELLS), 1.0, 6.0, ((1, 8), (2, 32)))
    intersection = draw_intersection(jax.random.fold_in(key_of[6], 71), 0)
    index_map = plant(jax.random.randint(key_of[2], (BLOCKS, P_SIZE), 0, SRC_DEV), jax.random.fold_in(key_of[2], 1), 0, SRC_DEV - 1).astype(jnp.int32)
    blocks = scatter_about(key_of[3], (BLOCKS, P_SIZE, TGT_DEV), (K * P_SIZE) ** -0.5, 0.125, ((0, 32),))
    bracket = plant(jax.random.randint(key_of[4], (LEVELS_OUT, TGT_CELLS), 0, LEVELS_IN - 1), jax.random.fold_in(key_of[4], 1), 0, (LEVELS_IN - 1) - 1).astype(jnp.int32)
    fraction = jnp.clip(1.0 * jax.random.uniform(key_of[5], (LEVELS_OUT, TGT_CELLS), jnp.float32) ** block_levels(key_of[5], (LEVELS_OUT, TGT_CELLS), ((1, 256),), -0.2, 0.2), 0.0, 1.0)
    return {"source_state": source_state, "intersection": intersection, "index_map": index_map, "blocks": blocks, "bracket": bracket, "fraction": fraction}


def reference(source_state, intersection, index_map, blocks, bracket, fraction):
    group_count = intersection.shape[0] // K
    fields_levels = F * LEVELS_IN
    source_tiles = jnp.transpose(source_state.reshape(fields_levels, group_count, SRC_DEV), (1, 0, 2))

    def remap_group(group_id):
        total_sum = jnp.zeros((fields_levels, TGT_DEV), jnp.float32)
        for block_slot in range(K):
            block_row = group_id * K + block_slot
            source_tile = source_tiles[intersection[block_row]]
            chosen = jnp.take(source_tile, index_map[block_row], axis=1).astype(jnp.float32)
            weights = blocks[block_row].astype(jnp.float32)
            total_sum = total_sum + jnp.dot(chosen, weights, preferred_element_type=jnp.float32)
        return total_sum.astype(jnp.bfloat16)

    remapped = lax.map(remap_group, jnp.arange(group_count, dtype=jnp.int32))
    horizontal = jnp.transpose(remapped, (1, 0, 2)).reshape(F, LEVELS_IN, group_count * TGT_DEV)
    widened = horizontal.astype(jnp.float32)
    below_level = jnp.take_along_axis(widened, bracket[None], axis=1)
    above_level = jnp.take_along_axis(widened, bracket[None] + 1, axis=1)
    upper_share = fraction[None]
    return ((1.0 - upper_share) * below_level + upper_share * above_level).astype(jnp.bfloat16)
```

```python
import functools

import jax
import jax.numpy as jnp
from jax import lax
from jax.experimental import pallas as pl
from jax.experimental.pallas import tpu as pltpu
from jax.sharding import PartitionSpec as P

MESH = pl.DeviceIdType.MESH
CHUNK = 256


def pick_rows(values, rows):
    return jnp.take_along_axis(values, rows, axis=0, mode="promise_in_bounds")


def kernel(
    groups,
    slabs,
    source_hbm,
    intersection_hbm,
    index_hbm,
    blocks_hbm,
    bracket_hbm,
    fraction_hbm,
    out_ref,
    source,
    intersection,
    index_map,
    weights,
    bracket_in,
    fraction_in,
    bracket,
    fraction,
    stacked,
    wanted,
    asked,
    picked,
    chosen,
    outbound,
    arrived,
    slab,
    total,
    local_sem,
    ask_send,
    ask_recv,
    value_send,
    value_recv,
    slab_send,
    slab_recv,
):
    group = lax.axis_index("horiz")
    place = lax.axis_index("lev")
    block_count = index_map.shape[0]
    depth = (block_count - 1) // 2
    fields, level_slab, tile_cells = source.shape
    rows = stacked.shape[0] // (tile_cells // CHUNK)
    even = level_slab - 1
    tail = fields * even
    columns = outbound.shape[2]
    offsets = [o for o in range(-depth, depth + 1) if o != 0]

    barrier = pltpu.get_barrier_semaphore()
    for offset in offsets:
        pl.semaphore_signal(
            barrier, inc=1, device_id={"horiz": lax.rem(group + offset + groups, groups)}, device_id_type=MESH
        )
    for step in range(1, slabs):
        pl.semaphore_signal(
            barrier, inc=1, device_id={"lev": lax.rem(place + step, slabs)}, device_id_type=MESH
        )

    loads = [
        pltpu.make_async_copy(src, dst, local_sem.at[n])
        for n, (src, dst) in enumerate(
            [
                (intersection_hbm, intersection),
                (index_hbm, index_map),
                (source_hbm, source),
                (bracket_hbm, bracket_in),
                (fraction_hbm, fraction_in),
                (blocks_hbm, weights),
            ]
        )
    ]
    for load in loads:
        load.start()
    loads[0].wait()
    loads[1].wait()

    for slot, offset in enumerate(range(-depth, depth + 1)):
        target = lax.rem(group + offset + groups, groups)
        row = jnp.zeros((1, index_map.shape[1]), jnp.int32)
        for block in range(block_count):
            row = row + jnp.where(intersection[block] == target, index_map[block : block + 1, :], 0)
        wanted[slot] = row

    pl.semaphore_wait(barrier, len(offsets) + slabs - 1)

    def ask(offset):
        slot = offset + depth
        return pltpu.make_async_remote_copy(
            src_ref=wanted.at[slot],
            dst_ref=asked.at[slot],
            send_sem=ask_send.at[slot],
            recv_sem=ask_recv.at[slot],
            device_id={"horiz": lax.rem(group + offset + groups, groups)},
            device_id_type=MESH,
        )

    def answer(offset):
        slot = offset + depth
        return pltpu.make_async_remote_copy(
            src_ref=picked.at[slot],
            dst_ref=chosen.at[slot],
            send_sem=value_send.at[slot],
            recv_sem=value_recv.at[slot],
            device_id={"horiz": lax.rem(group - offset + groups, groups)},
            device_id_type=MESH,
        )

    for offset in offsets:
        ask(offset).start()

    loads[2].wait()
    for chunk in range(tile_cells // CHUNK):
        cells = slice(chunk * CHUNK, (chunk + 1) * CHUNK)
        base = chunk * rows
        for field in range(fields):
            stacked[base + field * even : base + (field + 1) * even, :] = source[field, 0:even, cells]
        last = [source[field, even : even + 1, cells].astype(jnp.float32) for field in range(fields)]
        last.append(jnp.zeros((rows - tail - fields, CHUNK), jnp.float32))
        stacked[base + tail : base + rows, :] = jnp.concatenate(last, axis=0).astype(jnp.bfloat16)

    def select_cells(cell_ids):
        low = cell_ids & (CHUNK - 1)
        high = lax.shift_right_logical(cell_ids, CHUNK.bit_length() - 1)
        width = cell_ids.shape[1]
        picker = (
            (lax.broadcasted_iota(jnp.int32, (CHUNK, width), 0) == low).astype(jnp.float32).astype(jnp.bfloat16)
        )
        result = jnp.zeros((rows, width), jnp.float32)
        for chunk in range(tile_cells // CHUNK):
            part = jnp.dot(
                stacked[chunk * rows : (chunk + 1) * rows, :], picker, preferred_element_type=jnp.float32
            )
            result = jnp.where(high == chunk, part, result)
        return result.astype(jnp.bfloat16)

    chosen[depth] = select_cells(wanted[depth])
    for offset in offsets:
        slot = offset + depth
        ask(offset).wait_recv()
        picked[slot] = select_cells(asked[slot])
        answer(offset).start()

    loads[3].wait()
    loads[4].wait()
    levels_out = bracket_in.shape[0]
    bracket[bracket.shape[0] - 8 :, :] = jnp.zeros((8, columns), jnp.int32)
    fraction[fraction.shape[0] - 8 :, :] = jnp.zeros((8, columns), jnp.float32)
    bracket[0:levels_out, :] = bracket_in[...]
    fraction[0:levels_out, :] = fraction_in[...]
    total[...] = jnp.zeros_like(total)

    loads[5].wait()
    for offset in offsets:
        answer(offset).wait_recv()

    def deliver(step):
        return pltpu.make_async_remote_copy(
            src_ref=outbound.at[step],
            dst_ref=arrived.at[step],
            send_sem=slab_send.at[step],
            recv_sem=slab_recv.at[step],
            device_id={"lev": lax.rem(place + step, slabs)},
            device_id_type=MESH,
        )

    half = slabs // 2
    order = [half] + [s for d in range(half - 1, 0, -1) for s in (d, slabs - d)]
    positions = [
        jnp.minimum(lax.rem(intersection[b] - group + depth + groups, groups), block_count - 1)
        for b in range(block_count)
    ]
    for step in order + [0]:
        first = pl.multiple_of(lax.rem(place + step, slabs) * columns, columns)
        block = jnp.zeros((rows, columns), jnp.float32)
        for b in range(block_count):
            block = block + jnp.dot(
                chosen[positions[b]], weights[b, :, pl.ds(first, columns)], preferred_element_type=jnp.float32
            )
        if step == 0:
            arrived[0] = block.astype(jnp.bfloat16)
        else:
            outbound[step] = block.astype(jnp.bfloat16)
            deliver(step).start()

    for step in [0] + order:
        if step != 0:
            deliver(step).wait_recv()
        slab[...] = arrived[step].astype(jnp.float32)
        level0 = lax.rem(place - step + slabs, slabs) * level_slab

        for part in range(columns // 128):
            lanes = slice(part * 128, (part + 1) * 128)

            def mix(j, carry):
                out_rows = pl.ds(pl.multiple_of(j * 8, 8), 8)
                lower = bracket[out_rows, lanes] - level0
                upper = lower + 1
                share = fraction[out_rows, lanes]
                rest = 1.0 - share
                lower_tile, upper_tile = lower >> 3, upper >> 3
                lower_row, upper_row = lower & 7, upper & 7
                lower_last, upper_last = lower == even, upper == even
                for field in range(fields):
                    below = jnp.zeros((8, 128), jnp.float32)
                    above = jnp.zeros((8, 128), jnp.float32)
                    for tile in range(even // 8):
                        values = slab[field * even + tile * 8 : field * even + tile * 8 + 8, lanes]
                        below = jnp.where(lower_tile == tile, pick_rows(values, lower_row), below)
                        above = jnp.where(upper_tile == tile, pick_rows(values, upper_row), above)
                    last = slab[tail + field : tail + field + 1, lanes]
                    below = jnp.where(lower_last, last, below)
                    above = jnp.where(upper_last, last, above)
                    total[field, out_rows, lanes] += rest * below + share * above
                return carry

            lax.fori_loop(0, total.shape[1] // 8, mix, 0)

    out_ref[...] = total[:, 0:levels_out, :].astype(jnp.bfloat16)

    for offset in offsets:
        ask(offset).wait_send()
        answer(offset).wait_send()
    for step in order:
        deliver(step).wait_send()


def local(groups, slabs, source_state, intersection, index_map, blocks, bracket, fraction):
    fields, level_slab, tile_cells = source_state.shape
    block_count, width = index_map.shape
    levels_out, columns = bracket.shape
    rows = -(-fields * level_slab // 8) * 8
    out_rows = -(-levels_out // 8) * 8
    any_spec = pl.BlockSpec(memory_space=pl.ANY)
    dma = pltpu.SemaphoreType.DMA
    return pl.pallas_call(
        functools.partial(kernel, groups, slabs),
        out_shape=jax.ShapeDtypeStruct((fields, levels_out, columns), jnp.bfloat16),
        in_specs=[any_spec] * 6,
        out_specs=pl.BlockSpec(memory_space=pltpu.VMEM),
        scratch_shapes=[
            pltpu.VMEM(source_state.shape, jnp.bfloat16),
            pltpu.SMEM(intersection.shape, jnp.int32),
            pltpu.VMEM(index_map.shape, jnp.int32),
            pltpu.VMEM(blocks.shape, jnp.bfloat16),
            pltpu.VMEM(bracket.shape, jnp.int32),
            pltpu.VMEM(fraction.shape, jnp.float32),
            pltpu.VMEM((out_rows, columns), jnp.int32),
            pltpu.VMEM((out_rows, columns), jnp.float32),
            pltpu.VMEM((rows * (tile_cells // CHUNK), CHUNK), jnp.bfloat16),
            pltpu.VMEM((block_count, 1, width), jnp.int32),
            pltpu.VMEM((block_count, 1, width), jnp.int32),
            pltpu.VMEM((block_count, rows, width), jnp.bfloat16),
            pltpu.VMEM((block_count, rows, width), jnp.bfloat16),
            pltpu.VMEM((slabs, rows, columns), jnp.bfloat16),
            pltpu.VMEM((slabs, rows, columns), jnp.bfloat16),
            pltpu.VMEM((rows, columns), jnp.float32),
            pltpu.VMEM((fields, out_rows, columns), jnp.float32),
            dma((6,)),
            dma((block_count,)),
            dma((block_count,)),
            dma((block_count,)),
            dma((block_count,)),
            dma((slabs,)),
            dma((slabs,)),
        ],
        compiler_params=pltpu.CompilerParams(
            collective_id=0, has_side_effects=True, vmem_limit_bytes=56 * 1024 * 1024
        ),
        name="regrid",
    )(source_state, intersection, index_map, blocks, bracket, fraction)


def solution(mesh):
    in_specs = (
        P(None, "lev", "horiz"),
        P("horiz"),
        P("horiz", None),
        P("horiz", None, None),
        P(None, ("horiz", "lev")),
        P(None, ("horiz", "lev")),
    )
    out_specs = P(None, None, ("horiz", "lev"))
    body = functools.partial(local, mesh.shape["horiz"], mesh.shape["lev"])
    return jax.shard_map(body, mesh=mesh, in_specs=in_specs, out_specs=out_specs, check_vma=False)
```

```python
import functools

import jax
import jax.numpy as jnp
from jax import lax
from jax.experimental import pallas as pl
from jax.experimental.pallas import tpu as pltpu
from jax.sharding import PartitionSpec as P

MESH = pl.DeviceIdType.MESH
CHUNK = 256
TILE = 8


def pick_rows(values, rows):
    return jnp.take_along_axis(values, rows, axis=0, mode="promise_in_bounds")


def plan(fields, level_slab):
    tiles = level_slab // TILE
    odd = level_slab - tiles * TILE
    parts = []
    for tile in range(tiles):
        odd_rows = fields * odd if tile == tiles - 1 else 0
        parts.append((tile, fields * TILE, odd_rows, -(-(fields * TILE + odd_rows) // TILE) * TILE))
    return parts, odd


def kernel(
    groups,
    slabs,
    source_hbm,
    intersection_hbm,
    index_hbm,
    blocks_hbm,
    bracket_hbm,
    fraction_hbm,
    out_ref,
    source,
    intersection,
    index_map,
    weights,
    bracket_in,
    fraction_in,
    bracket,
    fraction,
    stacked,
    wanted,
    asked,
    picked,
    chosen,
    outbound,
    arrived,
    slab,
    total,
    local_sem,
    ask_send,
    ask_recv,
    value_send,
    value_recv,
    slab_send,
    slab_recv,
    rising,
    falling,
):
    group = lax.axis_index("horiz")
    place = lax.axis_index("lev")
    block_count = index_map.shape[0]
    depth = (block_count - 1) // 2
    fields, level_slab, tile_cells = source.shape
    chunks = tile_cells // CHUNK
    columns = bracket.shape[1]
    levels_out = bracket_in.shape[0]
    parts, odd = plan(fields, level_slab)
    tiles = len(parts)
    offsets = [sign * d for d in range(1, depth + 1) for sign in (-1, 1)]

    barrier = pltpu.get_barrier_semaphore()
    for offset in reversed(offsets):
        pl.semaphore_signal(
            barrier, inc=1, device_id={"horiz": lax.rem(group + offset + groups, groups)}, device_id_type=MESH
        )
    higher, lower_place = lax.rem(place + 1, slabs), lax.rem(place + slabs - 1, slabs)
    for neighbour in (higher, lower_place):
        pl.semaphore_signal(barrier, inc=1, device_id={"lev": neighbour}, device_id_type=MESH)

    loads = [
        pltpu.make_async_copy(src, dst, local_sem.at[n])
        for n, (src, dst) in enumerate(
            [
                (intersection_hbm, intersection),
                (index_hbm, index_map),
                (source_hbm, source),
                (bracket_hbm, bracket_in),
                (fraction_hbm, fraction_in),
                (blocks_hbm, weights),
            ]
        )
    ]
    for load in loads:
        load.start()
    loads[0].wait()
    loads[1].wait()

    for slot, offset in enumerate(range(-depth, depth + 1)):
        target = lax.rem(group + offset + groups, groups)
        row = jnp.zeros((1, index_map.shape[1]), jnp.int32)
        for block in range(block_count):
            row = row + jnp.where(intersection[block] == target, index_map[block : block + 1, :], 0)
        wanted[slot] = row

    pl.semaphore_wait(barrier, len(offsets) + 2)

    def ask(offset):
        slot = offset + depth
        return pltpu.make_async_remote_copy(
            src_ref=wanted.at[slot],
            dst_ref=asked.at[slot],
            send_sem=ask_send.at[slot],
            recv_sem=ask_recv.at[slot],
            device_id={"horiz": lax.rem(group + offset + groups, groups)},
            device_id_type=MESH,
        )

    def answer(part, offset):
        slot = offset + depth
        return pltpu.make_async_remote_copy(
            src_ref=picked[part].at[slot],
            dst_ref=chosen[part].at[slot],
            send_sem=value_send.at[part, slot],
            recv_sem=value_recv.at[part, slot],
            device_id={"horiz": lax.rem(group - offset + groups, groups)},
            device_id_type=MESH,
        )

    def deliver(part, step):
        return pltpu.make_async_remote_copy(
            src_ref=outbound[part].at[step],
            dst_ref=arrived[part].at[step],
            send_sem=slab_send.at[part, step],
            recv_sem=slab_recv.at[part, step],
            device_id={"lev": lax.rem(place + step, slabs)},
            device_id_type=MESH,
        )

    rounds = slabs // 2 - 1

    def tell(turn):
        pl.semaphore_signal(rising.at[turn], inc=1, device_id={"lev": higher}, device_id_type=MESH)
        pl.semaphore_signal(falling.at[turn], inc=1, device_id={"lev": lower_place}, device_id_type=MESH)

    def hear(turn):
        pl.semaphore_wait(rising.at[turn], 1)
        pl.semaphore_wait(falling.at[turn], 1)
        if turn + 1 < rounds:
            tell(turn + 1)

    for offset in reversed(offsets):
        ask(offset).start()
    tell(0)

    loads[2].wait()
    for part, (tile, full_rows, odd_rows, rows) in enumerate(parts):
        for chunk in range(chunks):
            cells = slice(chunk * CHUNK, (chunk + 1) * CHUNK)
            base = chunk * rows
            for field in range(fields):
                stacked[part][base + field * TILE : base + (field + 1) * TILE, :] = source[
                    field, tile * TILE : (tile + 1) * TILE, cells
                ]
            if odd_rows:
                last = [source[field, tiles * TILE :, cells].astype(jnp.float32) for field in range(fields)]
                last.append(jnp.zeros((rows - full_rows - odd_rows, CHUNK), jnp.float32))
                stacked[part][base + full_rows : base + rows, :] = jnp.concatenate(last, axis=0).astype(
                    jnp.bfloat16
                )

    def select_cells(part, cell_ids, result_ref):
        rows = parts[part][3]
        for piece in range(cell_ids.shape[1] // CHUNK):
            cells = slice(piece * CHUNK, (piece + 1) * CHUNK)
            low = cell_ids[:, cells] & (CHUNK - 1)
            high = lax.shift_right_logical(cell_ids[:, cells], CHUNK.bit_length() - 1)
            picker = (
                (lax.broadcasted_iota(jnp.int32, (CHUNK, CHUNK), 0) == low).astype(jnp.float32).astype(jnp.bfloat16)
            )
            found = jnp.dot(stacked[part][...], picker, preferred_element_type=jnp.float32)
            result = jnp.zeros((rows, CHUNK), jnp.float32)
            for chunk in range(chunks):
                result = jnp.where(high == chunk, found[chunk * rows : (chunk + 1) * rows], result)
            result_ref[:, cells] = result.astype(jnp.bfloat16)

    for part in range(tiles):
        select_cells(part, wanted[depth], chosen[part].at[depth])
    loads[3].wait()
    loads[4].wait()
    bracket[bracket.shape[0] - TILE :, :] = jnp.zeros((TILE, columns), jnp.int32)
    fraction[fraction.shape[0] - TILE :, :] = jnp.zeros((TILE, columns), jnp.float32)
    bracket[0:levels_out, :] = bracket_in[...]
    fraction[0:levels_out, :] = fraction_in[...]

    for part in range(tiles):
        for offset in offsets:
            slot = offset + depth
            if part == 0:
                ask(offset).wait_recv()
            select_cells(part, asked[slot], picked[part].at[slot])
            answer(part, offset).start()
        if part < rounds:
            hear(part)

    half = slabs // 2
    order = [half] + [s for d in range(half - 1, 0, -1) for s in (d, slabs - d)]
    positions = [
        jnp.minimum(lax.rem(intersection[b] - group + depth + groups, groups), block_count - 1)
        for b in range(block_count)
    ]
    loads[5].wait()
    for part in range(tiles):
        rows = parts[part][3]
        for offset in offsets:
            answer(part, offset).wait_recv()
        if part == 0:
            for turn in range(min(tiles, rounds), rounds):
                hear(turn)
        for step in order + [0]:
            first = pl.multiple_of(lax.rem(place + step, slabs) * columns, columns)
            block = jnp.zeros((rows, columns), jnp.float32)
            for b in range(block_count):
                block = block + jnp.dot(
                    chosen[part][positions[b]],
                    weights[b, :, pl.ds(first, columns)],
                    preferred_element_type=jnp.float32,
                )
            if step == 0:
                arrived[part][0] = block.astype(jnp.bfloat16)
            else:
                outbound[part][step] = block.astype(jnp.bfloat16)
                deliver(part, step).start()

    def blend(pairs, start):
        for part, step in pairs:
            slab[part][step] = arrived[part][step].astype(jnp.float32)

        def mix(j, carry):
            out_rows = pl.ds(pl.multiple_of(j * TILE, TILE), TILE)
            for piece in range(columns // 128):
                lanes = slice(piece * 128, (piece + 1) * 128)
                share = fraction[out_rows, lanes]
                rest = 1.0 - share
                below = [jnp.zeros((TILE, 128), jnp.float32)] * fields
                above = [jnp.zeros((TILE, 128), jnp.float32)] * fields
                for part, step in pairs:
                    tile, full_rows, odd_rows, rows = parts[part]
                    level0 = lax.rem(place - step + slabs, slabs) * level_slab
                    lower = bracket[out_rows, lanes] - level0
                    upper = lower + 1
                    in_lower, in_upper = (lower >> 3) == tile, (upper >> 3) == tile
                    lower_row, upper_row = lower & (TILE - 1), upper & (TILE - 1)
                    for field in range(fields):
                        values = slab[part][step, field * TILE : (field + 1) * TILE, lanes]
                        below[field] = jnp.where(in_lower, pick_rows(values, lower_row), below[field])
                        above[field] = jnp.where(in_upper, pick_rows(values, upper_row), above[field])
                    if odd_rows:
                        for extra in range(odd):
                            at_lower = lower == tiles * TILE + extra
                            at_upper = upper == tiles * TILE + extra
                            for field in range(fields):
                                row = full_rows + field * odd + extra
                                last = slab[part][step, row : row + 1, lanes]
                                below[field] = jnp.where(at_lower, last, below[field])
                                above[field] = jnp.where(at_upper, last, above[field])
                for field in range(fields):
                    mixed = rest * below[field] + share * above[field]
                    if start:
                        total[field, out_rows, lanes] = mixed
                    else:
                        total[field, out_rows, lanes] += mixed
            return carry

        lax.fori_loop(0, total.shape[1] // TILE, mix, 0)

    blend([(part, 0) for part in range(tiles)], True)
    ordered = [order[0:3]] + [order[n : n + 2] for n in range(3, len(order), 2)]
    for part in range(tiles):
        for steps in ordered:
            for step in steps:
                deliver(part, step).wait_recv()
            blend([(part, step) for step in steps], False)

    out_ref[...] = total[:, 0:levels_out, :].astype(jnp.bfloat16)

    for offset in offsets:
        ask(offset).wait_send()
        for part in range(tiles):
            answer(part, offset).wait_send()
    for step in order:
        for part in range(tiles):
            deliver(part, step).wait_send()


def local(groups, slabs, source_state, intersection, index_map, blocks, bracket, fraction):
    fields, level_slab, tile_cells = source_state.shape
    block_count, width = index_map.shape
    levels_out, columns = bracket.shape
    out_rows = -(-levels_out // TILE) * TILE
    chunks = tile_cells // CHUNK
    parts, _ = plan(fields, level_slab)
    rounds = slabs // 2 - 1
    any_spec = pl.BlockSpec(memory_space=pl.ANY)
    dma = pltpu.SemaphoreType.DMA

    def per_part(shape_of, dtype=jnp.bfloat16):
        return [pltpu.VMEM(shape_of(rows), dtype) for *_, rows in parts]

    return pl.pallas_call(
        functools.partial(kernel, groups, slabs),
        out_shape=pltpu.VMEM((fields, levels_out, columns), jnp.bfloat16),
        in_specs=[any_spec] * 6,
        out_specs=pl.BlockSpec(memory_space=pltpu.VMEM),
        scratch_shapes=[
            pltpu.VMEM(source_state.shape, jnp.bfloat16),
            pltpu.SMEM(intersection.shape, jnp.int32),
            pltpu.VMEM(index_map.shape, jnp.int32),
            pltpu.VMEM(blocks.shape, jnp.bfloat16),
            pltpu.VMEM(bracket.shape, jnp.int32),
            pltpu.VMEM(fraction.shape, jnp.float32),
            pltpu.VMEM((out_rows, columns), jnp.int32),
            pltpu.VMEM((out_rows, columns), jnp.float32),
            per_part(lambda rows: (rows * chunks, CHUNK)),
            pltpu.VMEM((block_count, 1, width), jnp.int32),
            pltpu.VMEM((block_count, 1, width), jnp.int32),
            per_part(lambda rows: (block_count, rows, width)),
            per_part(lambda rows: (block_count, rows, width)),
            per_part(lambda rows: (slabs, rows, columns)),
            per_part(lambda rows: (slabs, rows, columns)),
            per_part(lambda rows: (slabs, rows, columns), jnp.float32),
            pltpu.VMEM((fields, out_rows, columns), jnp.float32),
            dma((6,)),
            dma((block_count,)),
            dma((block_count,)),
            dma((len(parts), block_count)),
            dma((len(parts), block_count)),
            dma((len(parts), slabs)),
            dma((len(parts), slabs)),
            pltpu.SemaphoreType.REGULAR((rounds,)),
            pltpu.SemaphoreType.REGULAR((rounds,)),
        ],
        compiler_params=pltpu.CompilerParams(
            collective_id=0, has_side_effects=True, vmem_limit_bytes=56 * 1024 * 1024
        ),
        name="regrid",
    )(source_state, intersection, index_map, blocks, bracket, fraction)


def solution(mesh):
    in_specs = (
        P(None, "lev", "horiz"),
        P("horiz"),
        P("horiz", None),
        P("horiz", None, None),
        P(None, ("horiz", "lev")),
        P(None, ("horiz", "lev")),
    )
    out_specs = P(None, None, ("horiz", "lev"))
    body = functools.partial(local, mesh.shape["horiz"], mesh.shape["lev"])
    return jax.shard_map(body, mesh=mesh, in_specs=in_specs, out_specs=out_specs, check_vma=False)
```

```python
import functools

import jax
import jax.numpy as jnp
from jax import lax
from jax.experimental import pallas as pl
from jax.experimental.pallas import tpu as pltpu
from jax.sharding import PartitionSpec as P

MESH = pl.DeviceIdType.MESH
CHUNK = 256
TILE = 8


def pick_rows(values, rows):
    return jnp.take_along_axis(values, rows, axis=0, mode="promise_in_bounds")


def plan(fields, level_slab):
    tiles = level_slab // TILE
    odd = level_slab - tiles * TILE
    groups = [(0,)] + [tuple(range(f, min(f + 2, fields))) for f in range(1, fields, 2)]
    parts = []
    for number, members in enumerate(groups):
        full_rows = len(members) * tiles * TILE
        odd_rows = fields * odd if number == 0 else 0
        parts.append((members, full_rows, odd_rows, -(-(full_rows + odd_rows) // TILE) * TILE))
    return parts, tiles, odd


def kernel(
    groups,
    slabs,
    source_hbm,
    intersection_hbm,
    index_hbm,
    blocks_hbm,
    bracket_hbm,
    fraction_hbm,
    out_ref,
    source,
    intersection,
    index_map,
    weights,
    bracket_in,
    fraction_in,
    bracket,
    fraction,
    stacked,
    wanted,
    asked,
    picked,
    chosen,
    outbound,
    arrived,
    slab,
    total,
    local_sem,
    ask_send,
    ask_recv,
    value_send,
    value_recv,
    slab_send,
    slab_recv,
    rising,
    falling,
):
    group = lax.axis_index("horiz")
    place = lax.axis_index("lev")
    block_count = index_map.shape[0]
    depth = (block_count - 1) // 2
    fields, level_slab, tile_cells = source.shape
    chunks = tile_cells // CHUNK
    columns = bracket.shape[1]
    levels_out = bracket_in.shape[0]
    parts, tiles, odd = plan(fields, level_slab)
    offsets = list(range(1, depth + 1)) + list(range(-depth, 0))

    barrier = pltpu.get_barrier_semaphore()
    for offset in offsets:
        pl.semaphore_signal(
            barrier, inc=1, device_id={"horiz": lax.rem(group + offset + groups, groups)}, device_id_type=MESH
        )
    higher, lower_place = lax.rem(place + 1, slabs), lax.rem(place + slabs - 1, slabs)
    for neighbour in (higher, lower_place):
        pl.semaphore_signal(barrier, inc=1, device_id={"lev": neighbour}, device_id_type=MESH)

    loads = [
        pltpu.make_async_copy(src, dst, local_sem.at[n])
        for n, (src, dst) in enumerate(
            [
                (intersection_hbm, intersection),
                (index_hbm, index_map),
                (source_hbm, source),
                (bracket_hbm, bracket_in),
                (fraction_hbm, fraction_in),
                (blocks_hbm, weights),
            ]
        )
    ]
    for load in loads:
        load.start()
    loads[0].wait()
    loads[1].wait()

    for slot, offset in enumerate(range(-depth, depth + 1)):
        target = lax.rem(group + offset + groups, groups)
        row = jnp.zeros((1, index_map.shape[1]), jnp.int32)
        for block in range(block_count):
            row = row + jnp.where(intersection[block] == target, index_map[block : block + 1, :], 0)
        wanted[slot] = row

    pl.semaphore_wait(barrier, len(offsets) + 2)

    def ask(offset):
        slot = offset + depth
        return pltpu.make_async_remote_copy(
            src_ref=wanted.at[slot],
            dst_ref=asked.at[slot],
            send_sem=ask_send.at[slot],
            recv_sem=ask_recv.at[slot],
            device_id={"horiz": lax.rem(group + offset + groups, groups)},
            device_id_type=MESH,
        )

    def answer(part, offset):
        slot = offset + depth
        return pltpu.make_async_remote_copy(
            src_ref=picked[part].at[slot],
            dst_ref=chosen[part].at[slot],
            send_sem=value_send.at[part, slot],
            recv_sem=value_recv.at[part, slot],
            device_id={"horiz": lax.rem(group - offset + groups, groups)},
            device_id_type=MESH,
        )

    def deliver(part, step):
        return pltpu.make_async_remote_copy(
            src_ref=outbound[part].at[step],
            dst_ref=arrived[part].at[step],
            send_sem=slab_send.at[part, step],
            recv_sem=slab_recv.at[part, step],
            device_id={"lev": lax.rem(place + step, slabs)},
            device_id_type=MESH,
        )

    rounds = slabs // 2 - 1

    def tell(turn):
        pl.semaphore_signal(rising.at[turn], inc=1, device_id={"lev": higher}, device_id_type=MESH)
        pl.semaphore_signal(falling.at[turn], inc=1, device_id={"lev": lower_place}, device_id_type=MESH)

    def hear(turn):
        pl.semaphore_wait(rising.at[turn], 1)
        pl.semaphore_wait(falling.at[turn], 1)
        if turn + 1 < rounds:
            tell(turn + 1)

    for offset in offsets:
        ask(offset).start()
    tell(0)

    loads[2].wait()
    for part, (members, full_rows, odd_rows, rows) in enumerate(parts):
        for chunk in range(chunks):
            cells = slice(chunk * CHUNK, (chunk + 1) * CHUNK)
            base = chunk * rows
            for n, field in enumerate(members):
                stacked[part][base + n * tiles * TILE : base + (n + 1) * tiles * TILE, :] = source[
                    field, 0 : tiles * TILE, cells
                ]
            if odd_rows:
                last = [source[field, tiles * TILE :, cells].astype(jnp.float32) for field in range(fields)]
                last.append(jnp.zeros((rows - full_rows - odd_rows, CHUNK), jnp.float32))
                stacked[part][base + full_rows : base + rows, :] = jnp.concatenate(last, axis=0).astype(
                    jnp.bfloat16
                )

    def select_cells(part, cell_ids, result_ref):
        rows = parts[part][3]
        for piece in range(cell_ids.shape[1] // CHUNK):
            cells = slice(piece * CHUNK, (piece + 1) * CHUNK)
            low = cell_ids[:, cells] & (CHUNK - 1)
            high = lax.shift_right_logical(cell_ids[:, cells], CHUNK.bit_length() - 1)
            picker = (
                (lax.broadcasted_iota(jnp.int32, (CHUNK, CHUNK), 0) == low).astype(jnp.float32).astype(jnp.bfloat16)
            )
            found = jnp.dot(stacked[part][...], picker, preferred_element_type=jnp.float32)
            result = jnp.zeros((rows, CHUNK), jnp.float32)
            for chunk in range(chunks):
                result = jnp.where(high == chunk, found[chunk * rows : (chunk + 1) * rows], result)
            result_ref[:, cells] = result.astype(jnp.bfloat16)

    for part in range(len(parts)):
        select_cells(part, wanted[depth], chosen[part].at[depth])
    loads[3].wait()
    loads[4].wait()
    bracket[bracket.shape[0] - TILE :, :] = jnp.zeros((TILE, columns), jnp.int32)
    fraction[fraction.shape[0] - TILE :, :] = jnp.zeros((TILE, columns), jnp.float32)
    bracket[0:levels_out, :] = bracket_in[...]
    fraction[0:levels_out, :] = fraction_in[...]

    for part in range(len(parts)):
        for offset in offsets:
            slot = offset + depth
            if part == 0:
                ask(offset).wait_recv()
            select_cells(part, asked[slot], picked[part].at[slot])
            answer(part, offset).start()
        if part < rounds:
            hear(part)

    half = slabs // 2
    order = [half] + [s for d in range(half - 1, 0, -1) for s in (d, slabs - d)]
    positions = [
        jnp.minimum(lax.rem(intersection[b] - group + depth + groups, groups), block_count - 1)
        for b in range(block_count)
    ]
    loads[5].wait()
    for part in range(len(parts)):
        rows = parts[part][3]
        for offset in offsets:
            answer(part, offset).wait_recv()
        if part == 0:
            for turn in range(min(len(parts), rounds), rounds):
                hear(turn)
        for step in order + [0]:
            first = pl.multiple_of(lax.rem(place + step, slabs) * columns, columns)
            block = jnp.zeros((rows, columns), jnp.float32)
            for b in range(block_count):
                block = block + jnp.dot(
                    chosen[part][positions[b]],
                    weights[b, :, pl.ds(first, columns)],
                    preferred_element_type=jnp.float32,
                )
            if step == 0:
                arrived[part][0] = block.astype(jnp.bfloat16)
            else:
                outbound[part][step] = block.astype(jnp.bfloat16)
                deliver(part, step).start()

    def blend(part, steps, start):
        members, full_rows, odd_rows, rows = parts[part]
        touched = range(fields) if odd_rows else members
        for step in steps:
            slab[part][step] = arrived[part][step].astype(jnp.float32)

        def mix(j, carry):
            out_rows = pl.ds(pl.multiple_of(j * TILE, TILE), TILE)
            for piece in range(columns // 128):
                lanes = slice(piece * 128, (piece + 1) * 128)
                share = fraction[out_rows, lanes]
                rest = 1.0 - share
                below = {field: jnp.zeros((TILE, 128), jnp.float32) for field in touched}
                above = {field: jnp.zeros((TILE, 128), jnp.float32) for field in touched}
                for step in steps:
                    level0 = lax.rem(place - step + slabs, slabs) * level_slab
                    lower = bracket[out_rows, lanes] - level0
                    upper = lower + 1
                    lower_tile, upper_tile = lower >> 3, upper >> 3
                    lower_row, upper_row = lower & (TILE - 1), upper & (TILE - 1)
                    for tile in range(tiles):
                        in_lower, in_upper = lower_tile == tile, upper_tile == tile
                        for n, field in enumerate(members):
                            row = (n * tiles + tile) * TILE
                            values = slab[part][step, row : row + TILE, lanes]
                            below[field] = jnp.where(in_lower, pick_rows(values, lower_row), below[field])
                            above[field] = jnp.where(in_upper, pick_rows(values, upper_row), above[field])
                    if odd_rows:
                        for extra in range(odd):
                            at_lower = lower == tiles * TILE + extra
                            at_upper = upper == tiles * TILE + extra
                            for field in range(fields):
                                row = full_rows + field * odd + extra
                                last = slab[part][step, row : row + 1, lanes]
                                below[field] = jnp.where(at_lower, last, below[field])
                                above[field] = jnp.where(at_upper, last, above[field])
                for field in touched:
                    mixed = rest * below[field] + share * above[field]
                    if start:
                        total[field, out_rows, lanes] = mixed
                    else:
                        total[field, out_rows, lanes] += mixed
            return carry

        lax.fori_loop(0, total.shape[1] // TILE, mix, 0)

    for part in range(len(parts)):
        if part < len(parts) - 1:
            turns = [order]
        else:
            turns = [order[0:3]] + [order[n : n + 2] for n in range(3, len(order), 2)]
        for n, steps in enumerate(turns):
            for step in steps:
                deliver(part, step).wait_recv()
            blend(part, ([0] if n == 0 else []) + steps, part == 0)

    out_ref[...] = total[:, 0:levels_out, :].astype(jnp.bfloat16)

    for offset in offsets:
        ask(offset).wait_send()
        for part in range(len(parts)):
            answer(part, offset).wait_send()
    for step in order:
        for part in range(len(parts)):
            deliver(part, step).wait_send()


def local(groups, slabs, source_state, intersection, index_map, blocks, bracket, fraction):
    fields, level_slab, tile_cells = source_state.shape
    block_count, width = index_map.shape
    levels_out, columns = bracket.shape
    out_rows = -(-levels_out // TILE) * TILE
    chunks = tile_cells // CHUNK
    parts, _, _ = plan(fields, level_slab)
    rounds = slabs // 2 - 1
    any_spec = pl.BlockSpec(memory_space=pl.ANY)
    dma = pltpu.SemaphoreType.DMA

    def per_part(shape_of, dtype=jnp.bfloat16):
        return [pltpu.VMEM(shape_of(rows), dtype) for *_, rows in parts]

    return pl.pallas_call(
        functools.partial(kernel, groups, slabs),
        out_shape=pltpu.VMEM((fields, levels_out, columns), jnp.bfloat16),
        in_specs=[any_spec] * 6,
        out_specs=pl.BlockSpec(memory_space=pltpu.VMEM),
        scratch_shapes=[
            pltpu.VMEM(source_state.shape, jnp.bfloat16),
            pltpu.SMEM(intersection.shape, jnp.int32),
            pltpu.VMEM(index_map.shape, jnp.int32),
            pltpu.VMEM(blocks.shape, jnp.bfloat16),
            pltpu.VMEM(bracket.shape, jnp.int32),
            pltpu.VMEM(fraction.shape, jnp.float32),
            pltpu.VMEM((out_rows, columns), jnp.int32),
            pltpu.VMEM((out_rows, columns), jnp.float32),
            per_part(lambda rows: (rows * chunks, CHUNK)),
            pltpu.VMEM((block_count, 1, width), jnp.int32),
            pltpu.VMEM((block_count, 1, width), jnp.int32),
            per_part(lambda rows: (block_count, rows, width)),
            per_part(lambda rows: (block_count, rows, width)),
            per_part(lambda rows: (slabs, rows, columns)),
            per_part(lambda rows: (slabs, rows, columns)),
            per_part(lambda rows: (slabs, rows, columns), jnp.float32),
            pltpu.VMEM((fields, out_rows, columns), jnp.float32),
            dma((6,)),
            dma((block_count,)),
            dma((block_count,)),
            dma((len(parts), block_count)),
            dma((len(parts), block_count)),
            dma((len(parts), slabs)),
            dma((len(parts), slabs)),
            pltpu.SemaphoreType.REGULAR((rounds,)),
            pltpu.SemaphoreType.REGULAR((rounds,)),
        ],
        compiler_params=pltpu.CompilerParams(
            collective_id=0, has_side_effects=True, vmem_limit_bytes=56 * 1024 * 1024
        ),
        name="regrid",
    )(source_state, intersection, index_map, blocks, bracket, fraction)


def solution(mesh):
    in_specs = (
        P(None, "lev", "horiz"),
        P("horiz"),
        P("horiz", None),
        P("horiz", None, None),
        P(None, ("horiz", "lev")),
        P(None, ("horiz", "lev")),
    )
    out_specs = P(None, None, ("horiz", "lev"))
    body = functools.partial(local, mesh.shape["horiz"], mesh.shape["lev"])
    return jax.shard_map(body, mesh=mesh, in_specs=in_specs, out_specs=out_specs, check_vma=False)
```

```python
import functools

import jax
import jax.numpy as jnp
from jax import lax
from jax.experimental import pallas as pl
from jax.experimental.pallas import tpu as pltpu
from jax.sharding import PartitionSpec as P

MESH = pl.DeviceIdType.MESH
CHUNK = 256
TILE = 8


def pick_rows(values, rows):
    return jnp.take_along_axis(values, rows, axis=0, mode="promise_in_bounds")


def kernel(
    groups,
    slabs,
    source_hbm,
    intersection_hbm,
    index_hbm,
    blocks_hbm,
    bracket_hbm,
    fraction_hbm,
    out_ref,
    source,
    intersection,
    index_map,
    weights,
    bracket_in,
    fraction_in,
    bracket,
    fraction,
    stacked,
    wanted,
    asked,
    picked,
    chosen,
    outbound,
    arrived,
    slab,
    total,
    local_sem,
    ask_send,
    ask_recv,
    value_send,
    value_recv,
    slab_send,
    slab_recv,
    rising,
    falling,
):
    group = lax.axis_index("horiz")
    place = lax.axis_index("lev")
    block_count = index_map.shape[0]
    depth = (block_count - 1) // 2
    fields, level_slab, tile_cells = source.shape
    chunks = tile_cells // CHUNK
    columns = bracket.shape[1]
    levels_out = bracket_in.shape[0]
    tiles = level_slab // TILE
    odd = level_slab - tiles * TILE
    even = tiles * TILE
    full_rows = fields * even
    rows = stacked.shape[0] // chunks
    offsets = list(range(1, depth + 1)) + list(range(-depth, 0))

    barrier = pltpu.get_barrier_semaphore()
    for offset in offsets:
        pl.semaphore_signal(
            barrier, inc=1, device_id={"horiz": lax.rem(group + offset + groups, groups)}, device_id_type=MESH
        )
    higher, lower_place = lax.rem(place + 1, slabs), lax.rem(place + slabs - 1, slabs)
    for neighbour in (higher, lower_place):
        pl.semaphore_signal(barrier, inc=1, device_id={"lev": neighbour}, device_id_type=MESH)

    loads = [
        pltpu.make_async_copy(src, dst, local_sem.at[n])
        for n, (src, dst) in enumerate(
            [
                (intersection_hbm, intersection),
                (index_hbm, index_map),
                (source_hbm, source),
                (bracket_hbm, bracket_in),
                (fraction_hbm, fraction_in),
                (blocks_hbm, weights),
            ]
        )
    ]
    for load in loads:
        load.start()
    loads[0].wait()
    loads[1].wait()

    for slot, offset in enumerate(range(-depth, depth + 1)):
        target = lax.rem(group + offset + groups, groups)
        row = jnp.zeros((1, index_map.shape[1]), jnp.int32)
        for block in range(block_count):
            row = row + jnp.where(intersection[block] == target, index_map[block : block + 1, :], 0)
        wanted[slot] = row

    pl.semaphore_wait(barrier, len(offsets) + 2)

    def ask(offset):
        slot = offset + depth
        return pltpu.make_async_remote_copy(
            src_ref=wanted.at[slot],
            dst_ref=asked.at[slot],
            send_sem=ask_send.at[slot],
            recv_sem=ask_recv.at[slot],
            device_id={"horiz": lax.rem(group + offset + groups, groups)},
            device_id_type=MESH,
        )

    def answer(offset):
        slot = offset + depth
        return pltpu.make_async_remote_copy(
            src_ref=picked.at[slot],
            dst_ref=chosen.at[slot],
            send_sem=value_send.at[slot],
            recv_sem=value_recv.at[slot],
            device_id={"horiz": lax.rem(group - offset + groups, groups)},
            device_id_type=MESH,
        )

    def deliver(target):
        return pltpu.make_async_remote_copy(
            src_ref=outbound.at[target],
            dst_ref=arrived.at[place],
            send_sem=slab_send.at[target],
            recv_sem=slab_recv.at[place],
            device_id={"lev": target},
            device_id_type=MESH,
        )

    def await_slab(origin):
        pltpu.make_async_remote_copy(
            src_ref=outbound.at[origin],
            dst_ref=arrived.at[origin],
            send_sem=slab_send.at[origin],
            recv_sem=slab_recv.at[origin],
            device_id={"lev": origin},
            device_id_type=MESH,
        ).wait_recv()

    rounds = slabs // 2 - 1

    def tell(turn):
        pl.semaphore_signal(rising.at[turn], inc=1, device_id={"lev": higher}, device_id_type=MESH)
        pl.semaphore_signal(falling.at[turn], inc=1, device_id={"lev": lower_place}, device_id_type=MESH)

    def hear(turn):
        pl.semaphore_wait(rising.at[turn], 1)
        pl.semaphore_wait(falling.at[turn], 1)
        if turn + 1 < rounds:
            tell(turn + 1)

    for offset in offsets:
        ask(offset).start()
    tell(0)

    loads[2].wait()
    for chunk in range(chunks):
        cells = slice(chunk * CHUNK, (chunk + 1) * CHUNK)
        base = chunk * rows
        for field in range(fields):
            stacked[base + field * even : base + (field + 1) * even, :] = source[field, 0:even, cells]
        last = [source[field, even:, cells].astype(jnp.float32) for field in range(fields)]
        last.append(jnp.zeros((rows - full_rows - fields * odd, CHUNK), jnp.float32))
        stacked[base + full_rows : base + rows, :] = jnp.concatenate(last, axis=0).astype(jnp.bfloat16)

    def select_cells(cell_ids, result_ref):
        for piece in range(cell_ids.shape[1] // CHUNK):
            cells = slice(piece * CHUNK, (piece + 1) * CHUNK)
            low = cell_ids[:, cells] & (CHUNK - 1)
            high = lax.shift_right_logical(cell_ids[:, cells], CHUNK.bit_length() - 1)
            picker = (
                (lax.broadcasted_iota(jnp.int32, (CHUNK, CHUNK), 0) == low).astype(jnp.float32).astype(jnp.bfloat16)
            )
            found = jnp.dot(stacked[...], picker, preferred_element_type=jnp.float32)
            result = jnp.zeros((rows, CHUNK), jnp.float32)
            for chunk in range(chunks):
                result = jnp.where(high == chunk, found[chunk * rows : (chunk + 1) * rows], result)
            result_ref[:, cells] = result.astype(jnp.bfloat16)

    select_cells(wanted[depth], chosen.at[depth])
    loads[3].wait()
    loads[4].wait()
    bracket[bracket.shape[0] - TILE :, :] = jnp.zeros((TILE, columns), jnp.int32)
    fraction[fraction.shape[0] - TILE :, :] = jnp.zeros((TILE, columns), jnp.float32)
    bracket[0:levels_out, :] = bracket_in[...]
    fraction[0:levels_out, :] = fraction_in[...]

    for turn, offset in enumerate(offsets):
        slot = offset + depth
        ask(offset).wait_recv()
        select_cells(asked[slot], picked.at[slot])
        answer(offset).start()
        if turn % 2 == 1 and turn // 2 < rounds - 1:
            hear(turn // 2)

    half = slabs // 2
    order = [0] + [p for d in range(1, half) for p in (d, slabs - d)] + [half]
    positions = [
        jnp.minimum(lax.rem(intersection[b] - group + depth + groups, groups), block_count - 1)
        for b in range(block_count)
    ]
    loads[5].wait()
    for offset in offsets:
        answer(offset).wait_recv()
    for turn in range(min(len(offsets) // 2, rounds - 1), rounds):
        hear(turn)
    for target in order:
        block = jnp.zeros((rows, columns), jnp.float32)
        for b in range(block_count):
            block = block + jnp.dot(
                chosen[positions[b]],
                weights[b, :, target * columns : (target + 1) * columns],
                preferred_element_type=jnp.float32,
            )
        outbound[target] = block.astype(jnp.bfloat16)

        @pl.when(target == place)
        def _():
            arrived[target] = outbound[target]

        @pl.when(target != place)
        def _():
            deliver(target).start()

    def blend(origins, start):
        for origin in origins:
            slab[origin] = arrived[origin].astype(jnp.float32)

        def mix(j, carry):
            out_rows = pl.ds(pl.multiple_of(j * TILE, TILE), TILE)
            for piece in range(columns // 128):
                lanes = slice(piece * 128, (piece + 1) * 128)
                share = fraction[out_rows, lanes]
                rest = 1.0 - share
                below = [jnp.zeros((TILE, 128), jnp.float32)] * fields
                above = [jnp.zeros((TILE, 128), jnp.float32)] * fields
                for origin in origins:
                    lower = bracket[out_rows, lanes] - origin * level_slab
                    upper = lower + 1
                    lower_tile, upper_tile = lower >> 3, upper >> 3
                    lower_row, upper_row = lower & (TILE - 1), upper & (TILE - 1)
                    for tile in range(tiles):
                        in_lower, in_upper = lower_tile == tile, upper_tile == tile
                        for field in range(fields):
                            row = field * even + tile * TILE
                            values = slab[origin, row : row + TILE, lanes]
                            below[field] = jnp.where(in_lower, pick_rows(values, lower_row), below[field])
                            above[field] = jnp.where(in_upper, pick_rows(values, upper_row), above[field])
                    for extra in range(odd):
                        at_lower, at_upper = lower == even + extra, upper == even + extra
                        for field in range(fields):
                            row = full_rows + field * odd + extra
                            last = slab[origin, row : row + 1, lanes]
                            below[field] = jnp.where(at_lower, last, below[field])
                            above[field] = jnp.where(at_upper, last, above[field])
                for field in range(fields):
                    mixed = rest * below[field] + share * above[field]
                    if start:
                        total[field, out_rows, lanes] = mixed
                    else:
                        total[field, out_rows, lanes] += mixed
            return carry

        lax.fori_loop(0, total.shape[1] // TILE, mix, 0)

    turns = [order[0:3]] + [order[n : n + 2] for n in range(3, len(order), 2)]
    for n, origins in enumerate(turns):
        for origin in origins:

            @pl.when(origin != place)
            def _():
                await_slab(origin)

        blend(origins, n == 0)

    out_ref[...] = total[:, 0:levels_out, :].astype(jnp.bfloat16)

    for offset in offsets:
        ask(offset).wait_send()
        answer(offset).wait_send()
    for target in order:

        @pl.when(target != place)
        def _():
            deliver(target).wait_send()


def local(groups, slabs, source_state, intersection, index_map, blocks, bracket, fraction):
    fields, level_slab, tile_cells = source_state.shape
    block_count, width = index_map.shape
    levels_out, columns = bracket.shape
    out_rows = -(-levels_out // TILE) * TILE
    chunks = tile_cells // CHUNK
    rows = -(-fields * level_slab // TILE) * TILE
    rounds = slabs // 2 - 1
    any_spec = pl.BlockSpec(memory_space=pl.ANY)
    dma = pltpu.SemaphoreType.DMA

    return pl.pallas_call(
        functools.partial(kernel, groups, slabs),
        out_shape=pltpu.VMEM((fields, levels_out, columns), jnp.bfloat16),
        in_specs=[any_spec] * 6,
        out_specs=pl.BlockSpec(memory_space=pltpu.VMEM),
        scratch_shapes=[
            pltpu.VMEM(source_state.shape, jnp.bfloat16),
            pltpu.SMEM(intersection.shape, jnp.int32),
            pltpu.VMEM(index_map.shape, jnp.int32),
            pltpu.VMEM(blocks.shape, jnp.bfloat16),
            pltpu.VMEM(bracket.shape, jnp.int32),
            pltpu.VMEM(fraction.shape, jnp.float32),
            pltpu.VMEM((out_rows, columns), jnp.int32),
            pltpu.VMEM((out_rows, columns), jnp.float32),
            pltpu.VMEM((rows * chunks, CHUNK), jnp.bfloat16),
            pltpu.VMEM((block_count, 1, width), jnp.int32),
            pltpu.VMEM((block_count, 1, width), jnp.int32),
            pltpu.VMEM((block_count, rows, width), jnp.bfloat16),
            pltpu.VMEM((block_count, rows, width), jnp.bfloat16),
            pltpu.VMEM((slabs, rows, columns), jnp.bfloat16),
            pltpu.VMEM((slabs, rows, columns), jnp.bfloat16),
            pltpu.VMEM((slabs, rows, columns), jnp.float32),
            pltpu.VMEM((fields, out_rows, columns), jnp.float32),
            dma((6,)),
            dma((block_count,)),
            dma((block_count,)),
            dma((block_count,)),
            dma((block_count,)),
            dma((slabs,)),
            dma((slabs,)),
            pltpu.SemaphoreType.REGULAR((rounds,)),
            pltpu.SemaphoreType.REGULAR((rounds,)),
        ],
        compiler_params=pltpu.CompilerParams(
            collective_id=0, has_side_effects=True, vmem_limit_bytes=56 * 1024 * 1024
        ),
        name="regrid",
    )(source_state, intersection, index_map, blocks, bracket, fraction)


def solution(mesh):
    in_specs = (
        P(None, "lev", "horiz"),
        P("horiz"),
        P("horiz", None),
        P("horiz", None, None),
        P(None, ("horiz", "lev")),
        P(None, ("horiz", "lev")),
    )
    out_specs = P(None, None, ("horiz", "lev"))
    body = functools.partial(local, mesh.shape["horiz"], mesh.shape["lev"])
    return jax.shard_map(body, mesh=mesh, in_specs=in_specs, out_specs=out_specs, check_vma=False)
```

```python
import functools

import jax
import jax.numpy as jnp
from jax import lax
from jax.experimental import pallas as pl
from jax.experimental.pallas import tpu as pltpu
from jax.sharding import PartitionSpec as P

MESH = pl.DeviceIdType.MESH
CHUNK = 256
TILE = 8


def pick_rows(values, rows):
    return jnp.take_along_axis(values, rows, axis=0, mode="promise_in_bounds")


def kernel(
    groups,
    slabs,
    source_hbm,
    intersection_hbm,
    index_hbm,
    blocks_hbm,
    bracket_hbm,
    fraction_hbm,
    out_ref,
    source,
    intersection,
    index_map,
    weights,
    bracket_in,
    fraction_in,
    bracket,
    fraction,
    stacked,
    wanted,
    asked,
    picked,
    chosen,
    outbound,
    arrived,
    slab,
    total,
    local_sem,
    ask_send,
    ask_recv,
    value_send,
    value_recv,
    slab_send,
    slab_recv,
    rising,
    falling,
):
    group = lax.axis_index("horiz")
    place = lax.axis_index("lev")
    block_count = index_map.shape[0]
    depth = (block_count - 1) // 2
    fields, level_slab, tile_cells = source.shape
    chunks = tile_cells // CHUNK
    columns = bracket.shape[1]
    levels_out = bracket_in.shape[0]
    tiles = level_slab // TILE
    odd = level_slab - tiles * TILE
    even = tiles * TILE
    full_rows = fields * even
    rows = stacked.shape[0] // chunks
    offsets = list(range(1, depth + 1)) + list(range(-1, -depth - 1, -1))

    barrier = pltpu.get_barrier_semaphore()
    for offset in offsets:
        pl.semaphore_signal(
            barrier, inc=1, device_id={"horiz": lax.rem(group + offset + groups, groups)}, device_id_type=MESH
        )
    higher, lower_place = lax.rem(place + 1, slabs), lax.rem(place + slabs - 1, slabs)
    for neighbour in (higher, lower_place):
        pl.semaphore_signal(barrier, inc=1, device_id={"lev": neighbour}, device_id_type=MESH)

    loads = [
        pltpu.make_async_copy(src, dst, local_sem.at[n])
        for n, (src, dst) in enumerate(
            [
                (intersection_hbm, intersection),
                (index_hbm, index_map),
                (source_hbm, source),
                (bracket_hbm, bracket_in),
                (fraction_hbm, fraction_in),
                (blocks_hbm, weights),
            ]
        )
    ]
    for load in loads:
        load.start()
    loads[0].wait()
    loads[1].wait()

    for slot, offset in enumerate(range(-depth, depth + 1)):
        target = lax.rem(group + offset + groups, groups)
        row = jnp.zeros((1, index_map.shape[1]), jnp.int32)
        for block in range(block_count):
            row = row + jnp.where(intersection[block] == target, index_map[block : block + 1, :], 0)
        wanted[slot] = row

    pl.semaphore_wait(barrier, len(offsets) + 2)

    def ask(offset):
        slot = offset + depth
        return pltpu.make_async_remote_copy(
            src_ref=wanted.at[slot],
            dst_ref=asked.at[slot],
            send_sem=ask_send.at[slot],
            recv_sem=ask_recv.at[slot],
            device_id={"horiz": lax.rem(group + offset + groups, groups)},
            device_id_type=MESH,
        )

    def answer(offset):
        slot = offset + depth
        return pltpu.make_async_remote_copy(
            src_ref=picked.at[slot],
            dst_ref=chosen.at[slot],
            send_sem=value_send.at[slot],
            recv_sem=value_recv.at[slot],
            device_id={"horiz": lax.rem(group - offset + groups, groups)},
            device_id_type=MESH,
        )

    def deliver(target):
        return pltpu.make_async_remote_copy(
            src_ref=outbound.at[target],
            dst_ref=arrived.at[place],
            send_sem=slab_send.at[target],
            recv_sem=slab_recv.at[place],
            device_id={"lev": target},
            device_id_type=MESH,
        )

    def await_slab(origin):
        pltpu.make_async_remote_copy(
            src_ref=outbound.at[origin],
            dst_ref=arrived.at[origin],
            send_sem=slab_send.at[origin],
            recv_sem=slab_recv.at[origin],
            device_id={"lev": origin},
            device_id_type=MESH,
        ).wait_recv()

    rounds = slabs // 2 - 1

    def tell(turn):
        pl.semaphore_signal(rising.at[turn], inc=1, device_id={"lev": higher}, device_id_type=MESH)
        pl.semaphore_signal(falling.at[turn], inc=1, device_id={"lev": lower_place}, device_id_type=MESH)

    def hear(turn):
        pl.semaphore_wait(rising.at[turn], 1)
        pl.semaphore_wait(falling.at[turn], 1)
        if turn + 1 < rounds:
            tell(turn + 1)

    for offset in offsets:
        ask(offset).start()
    tell(0)

    loads[2].wait()
    for chunk in range(chunks):
        cells = slice(chunk * CHUNK, (chunk + 1) * CHUNK)
        base = chunk * rows
        for field in range(fields):
            stacked[base + field * even : base + (field + 1) * even, :] = source[field, 0:even, cells]
        last = [source[field, even:, cells].astype(jnp.float32) for field in range(fields)]
        last.append(jnp.zeros((rows - full_rows - fields * odd, CHUNK), jnp.float32))
        stacked[base + full_rows : base + rows, :] = jnp.concatenate(last, axis=0).astype(jnp.bfloat16)

    def select_cells(cell_ids, result_ref):
        for piece in range(cell_ids.shape[1] // CHUNK):
            cells = slice(piece * CHUNK, (piece + 1) * CHUNK)
            low = cell_ids[:, cells] & (CHUNK - 1)
            high = lax.shift_right_logical(cell_ids[:, cells], CHUNK.bit_length() - 1)
            picker = (
                (lax.broadcasted_iota(jnp.int32, (CHUNK, CHUNK), 0) == low).astype(jnp.float32).astype(jnp.bfloat16)
            )
            found = jnp.dot(stacked[...], picker, preferred_element_type=jnp.float32)
            result = jnp.zeros((rows, CHUNK), jnp.float32)
            for chunk in range(chunks):
                result = jnp.where(high == chunk, found[chunk * rows : (chunk + 1) * rows], result)
            result_ref[:, cells] = result.astype(jnp.bfloat16)

    select_cells(wanted[depth], chosen.at[depth])
    loads[3].wait()
    loads[4].wait()
    bracket[bracket.shape[0] - TILE :, :] = jnp.zeros((TILE, columns), jnp.int32)
    fraction[fraction.shape[0] - TILE :, :] = jnp.zeros((TILE, columns), jnp.float32)
    bracket[0:levels_out, :] = bracket_in[...]
    fraction[0:levels_out, :] = fraction_in[...]

    for turn, offset in enumerate(offsets):
        slot = offset + depth
        ask(offset).wait_recv()
        select_cells(asked[slot], picked.at[slot])
        answer(offset).start()
        if turn % 2 == 1 and turn // 2 < rounds - 1:
            hear(turn // 2)

    order = list(range(slabs))
    awaited = order[: slabs // 2] + order[: slabs // 2 - 1 : -1]
    positions = [
        jnp.minimum(lax.rem(intersection[b] - group + depth + groups, groups), block_count - 1)
        for b in range(block_count)
    ]
    loads[5].wait()
    for offset in offsets:
        answer(offset).wait_recv()
    for turn in range(min(len(offsets) // 2, rounds - 1), rounds):
        hear(turn)
    for target in order:
        block = jnp.zeros((rows, columns), jnp.float32)
        for b in range(block_count):
            block = block + jnp.dot(
                chosen[positions[b]],
                weights[b, :, target * columns : (target + 1) * columns],
                preferred_element_type=jnp.float32,
            )
        outbound[target] = block.astype(jnp.bfloat16)

        @pl.when(target == place)
        def _():
            arrived[target] = outbound[target]

        @pl.when(target != place)
        def _():
            deliver(target).start()

    def blend(origins, start):
        for origin in origins:
            slab[origin] = arrived[origin].astype(jnp.float32)

        def mix(j, carry):
            out_rows = pl.ds(pl.multiple_of(j * TILE, TILE), TILE)
            for piece in range(columns // 128):
                lanes = slice(piece * 128, (piece + 1) * 128)
                share = fraction[out_rows, lanes]
                rest = 1.0 - share
                below = [jnp.zeros((TILE, 128), jnp.float32)] * fields
                above = [jnp.zeros((TILE, 128), jnp.float32)] * fields
                for origin in origins:
                    lower = bracket[out_rows, lanes] - origin * level_slab
                    upper = lower + 1
                    lower_tile, upper_tile = lower >> 3, upper >> 3
                    lower_row, upper_row = lower & (TILE - 1), upper & (TILE - 1)
                    for tile in range(tiles):
                        in_lower, in_upper = lower_tile == tile, upper_tile == tile
                        for field in range(fields):
                            row = field * even + tile * TILE
                            values = slab[origin, row : row + TILE, lanes]
                            below[field] = jnp.where(in_lower, pick_rows(values, lower_row), below[field])
                            above[field] = jnp.where(in_upper, pick_rows(values, upper_row), above[field])
                    for extra in range(odd):
                        at_lower, at_upper = lower == even + extra, upper == even + extra
                        for field in range(fields):
                            row = full_rows + field * odd + extra
                            last = slab[origin, row : row + 1, lanes]
                            below[field] = jnp.where(at_lower, last, below[field])
                            above[field] = jnp.where(at_upper, last, above[field])
                for field in range(fields):
                    mixed = rest * below[field] + share * above[field]
                    if start:
                        total[field, out_rows, lanes] = mixed
                    else:
                        total[field, out_rows, lanes] += mixed
            return carry

        lax.fori_loop(0, total.shape[1] // TILE, mix, 0)

    turns = [awaited[0:3]] + [awaited[n : n + 2] for n in range(3, slabs, 2)]
    for n, origins in enumerate(turns):
        for origin in origins:

            @pl.when(origin != place)
            def _():
                await_slab(origin)

        blend(origins, n == 0)

    out_ref[...] = total[:, 0:levels_out, :].astype(jnp.bfloat16)

    for offset in offsets:
        ask(offset).wait_send()
        answer(offset).wait_send()
    for target in order:

        @pl.when(target != place)
        def _():
            deliver(target).wait_send()


def local(groups, slabs, source_state, intersection, index_map, blocks, bracket, fraction):
    fields, level_slab, tile_cells = source_state.shape
    block_count, width = index_map.shape
    levels_out, columns = bracket.shape
    out_rows = -(-levels_out // TILE) * TILE
    chunks = tile_cells // CHUNK
    rows = -(-fields * level_slab // TILE) * TILE
    rounds = slabs // 2 - 1
    any_spec = pl.BlockSpec(memory_space=pl.ANY)
    dma = pltpu.SemaphoreType.DMA

    return pl.pallas_call(
        functools.partial(kernel, groups, slabs),
        out_shape=pltpu.VMEM((fields, levels_out, columns), jnp.bfloat16),
        in_specs=[any_spec] * 6,
        out_specs=pl.BlockSpec(memory_space=pltpu.VMEM),
        scratch_shapes=[
            pltpu.VMEM(source_state.shape, jnp.bfloat16),
            pltpu.SMEM(intersection.shape, jnp.int32),
            pltpu.VMEM(index_map.shape, jnp.int32),
            pltpu.VMEM(blocks.shape, jnp.bfloat16),
            pltpu.VMEM(bracket.shape, jnp.int32),
            pltpu.VMEM(fraction.shape, jnp.float32),
            pltpu.VMEM((out_rows, columns), jnp.int32),
            pltpu.VMEM((out_rows, columns), jnp.float32),
            pltpu.VMEM((rows * chunks, CHUNK), jnp.bfloat16),
            pltpu.VMEM((block_count, 1, width), jnp.int32),
            pltpu.VMEM((block_count, 1, width), jnp.int32),
            pltpu.VMEM((block_count, rows, width), jnp.bfloat16),
            pltpu.VMEM((block_count, rows, width), jnp.bfloat16),
            pltpu.VMEM((slabs, rows, columns), jnp.bfloat16),
            pltpu.VMEM((slabs, rows, columns), jnp.bfloat16),
            pltpu.VMEM((slabs, rows, columns), jnp.float32),
            pltpu.VMEM((fields, out_rows, columns), jnp.float32),
            dma((6,)),
            dma((block_count,)),
            dma((block_count,)),
            dma((block_count,)),
            dma((block_count,)),
            dma((slabs,)),
            dma((slabs,)),
            pltpu.SemaphoreType.REGULAR((rounds,)),
            pltpu.SemaphoreType.REGULAR((rounds,)),
        ],
        compiler_params=pltpu.CompilerParams(
            collective_id=0, has_side_effects=True, vmem_limit_bytes=56 * 1024 * 1024
        ),
        name="regrid",
    )(source_state, intersection, index_map, blocks, bracket, fraction)


def solution(mesh):
    in_specs = (
        P(None, "lev", "horiz"),
        P("horiz"),
        P("horiz", None),
        P("horiz", None, None),
        P(None, ("horiz", "lev")),
        P(None, ("horiz", "lev")),
    )
    out_specs = P(None, None, ("horiz", "lev"))
    body = functools.partial(local, mesh.shape["horiz"], mesh.shape["lev"])
    return jax.shard_map(body, mesh=mesh, in_specs=in_specs, out_specs=out_specs, check_vma=False)
```

```python
import functools

import jax
import jax.numpy as jnp
from jax import lax
from jax.experimental import pallas as pl
from jax.experimental.pallas import tpu as pltpu
from jax.sharding import PartitionSpec as P

MESH = pl.DeviceIdType.MESH
CHUNK = 256
TILE = 8


def pick_rows(values, rows):
    return jnp.take_along_axis(values, rows, axis=0, mode="promise_in_bounds")


def kernel(
    groups,
    slabs,
    source_hbm,
    intersection_hbm,
    index_hbm,
    blocks_hbm,
    bracket_hbm,
    fraction_hbm,
    out_ref,
    source,
    intersection,
    index_map,
    weights,
    bracket_in,
    fraction_in,
    bracket,
    fraction,
    stacked,
    wanted,
    asked,
    picked,
    chosen,
    outbound,
    arrived,
    slab,
    total,
    local_sem,
    ask_send,
    ask_recv,
    value_send,
    value_recv,
    slab_send,
    slab_recv,
    rising,
    falling,
):
    group = lax.axis_index("horiz")
    place = lax.axis_index("lev")
    block_count = index_map.shape[0]
    depth = (block_count - 1) // 2
    fields, level_slab, tile_cells = source.shape
    chunks = tile_cells // CHUNK
    columns = bracket.shape[1]
    levels_out = bracket_in.shape[0]
    tiles = level_slab // TILE
    odd = level_slab - tiles * TILE
    even = tiles * TILE
    full_rows = fields * even
    rows = stacked.shape[0] // chunks
    offsets = list(range(1, depth + 1)) + list(range(-depth, 0))

    barrier = pltpu.get_barrier_semaphore()
    for offset in offsets:
        pl.semaphore_signal(
            barrier, inc=1, device_id={"horiz": lax.rem(group + offset + groups, groups)}, device_id_type=MESH
        )
    higher, lower_place = lax.rem(place + 1, slabs), lax.rem(place + slabs - 1, slabs)
    for neighbour in (higher, lower_place):
        pl.semaphore_signal(barrier, inc=1, device_id={"lev": neighbour}, device_id_type=MESH)

    loads = [
        pltpu.make_async_copy(src, dst, local_sem.at[n])
        for n, (src, dst) in enumerate(
            [
                (intersection_hbm, intersection),
                (index_hbm, index_map),
                (source_hbm, source),
                (bracket_hbm, bracket_in),
                (fraction_hbm, fraction_in),
                (blocks_hbm, weights),
            ]
        )
    ]
    for load in loads:
        load.start()
    loads[0].wait()
    loads[1].wait()

    for slot, offset in enumerate(range(-depth, depth + 1)):
        target = lax.rem(group + offset + groups, groups)
        row = jnp.zeros((1, index_map.shape[1]), jnp.int32)
        for block in range(block_count):
            row = row + jnp.where(intersection[block] == target, index_map[block : block + 1, :], 0)
        wanted[slot] = row

    pl.semaphore_wait(barrier, len(offsets) + 2)

    def ask(offset):
        slot = offset + depth
        return pltpu.make_async_remote_copy(
            src_ref=wanted.at[slot],
            dst_ref=asked.at[slot],
            send_sem=ask_send.at[slot],
            recv_sem=ask_recv.at[slot],
            device_id={"horiz": lax.rem(group + offset + groups, groups)},
            device_id_type=MESH,
        )

    def answer(offset):
        slot = offset + depth
        return pltpu.make_async_remote_copy(
            src_ref=picked.at[slot],
            dst_ref=chosen.at[slot],
            send_sem=value_send.at[slot],
            recv_sem=value_recv.at[slot],
            device_id={"horiz": lax.rem(group - offset + groups, groups)},
            device_id_type=MESH,
        )

    def deliver(target):
        return pltpu.make_async_remote_copy(
            src_ref=outbound.at[target],
            dst_ref=arrived.at[place],
            send_sem=slab_send.at[target],
            recv_sem=slab_recv.at[place],
            device_id={"lev": target},
            device_id_type=MESH,
        )

    def await_slab(origin):
        pltpu.make_async_remote_copy(
            src_ref=outbound.at[origin],
            dst_ref=arrived.at[origin],
            send_sem=slab_send.at[origin],
            recv_sem=slab_recv.at[origin],
            device_id={"lev": origin},
            device_id_type=MESH,
        ).wait_recv()

    rounds = slabs // 2 - 1

    def tell(turn):
        pl.semaphore_signal(rising.at[turn], inc=1, device_id={"lev": higher}, device_id_type=MESH)
        pl.semaphore_signal(falling.at[turn], inc=1, device_id={"lev": lower_place}, device_id_type=MESH)

    def hear(turn):
        pl.semaphore_wait(rising.at[turn], 1)
        pl.semaphore_wait(falling.at[turn], 1)
        if turn + 1 < rounds:
            tell(turn + 1)

    for offset in offsets:
        ask(offset).start()
    tell(0)

    loads[2].wait()
    for chunk in range(chunks):
        cells = slice(chunk * CHUNK, (chunk + 1) * CHUNK)
        base = chunk * rows
        for field in range(fields):
            stacked[base + field * even : base + (field + 1) * even, :] = source[field, 0:even, cells]
        last = [source[field, even:, cells].astype(jnp.float32) for field in range(fields)]
        last.append(jnp.zeros((rows - full_rows - fields * odd, CHUNK), jnp.float32))
        stacked[base + full_rows : base + rows, :] = jnp.concatenate(last, axis=0).astype(jnp.bfloat16)

    def select_cells(cell_ids, result_ref):
        for piece in range(cell_ids.shape[1] // CHUNK):
            cells = slice(piece * CHUNK, (piece + 1) * CHUNK)
            low = cell_ids[:, cells] & (CHUNK - 1)
            high = lax.shift_right_logical(cell_ids[:, cells], CHUNK.bit_length() - 1)
            picker = (
                (lax.broadcasted_iota(jnp.int32, (CHUNK, CHUNK), 0) == low).astype(jnp.float32).astype(jnp.bfloat16)
            )
            found = jnp.dot(stacked[...], picker, preferred_element_type=jnp.float32)
            result = jnp.zeros((rows, CHUNK), jnp.float32)
            for chunk in range(chunks):
                result = jnp.where(high == chunk, found[chunk * rows : (chunk + 1) * rows], result)
            result_ref[:, cells] = result.astype(jnp.bfloat16)

    select_cells(wanted[depth], chosen.at[depth])
    loads[3].wait()
    loads[4].wait()
    bracket[bracket.shape[0] - TILE :, :] = jnp.zeros((TILE, columns), jnp.int32)
    fraction[fraction.shape[0] - TILE :, :] = jnp.zeros((TILE, columns), jnp.float32)
    bracket[0:levels_out, :] = bracket_in[...]
    fraction[0:levels_out, :] = fraction_in[...]

    for turn, offset in enumerate(offsets):
        slot = offset + depth
        ask(offset).wait_recv()
        select_cells(asked[slot], picked.at[slot])
        answer(offset).start()
        if turn % 2 == 1 and turn // 2 < rounds - 1:
            hear(turn // 2)

    core = lax.rem(group, 2)
    orders = zip([1, 2, 0, 3, 7, 4, 6, 5], [0, 1, 7, 2, 6, 3, 5, 4])
    order = [early * core + late * (1 - core) for late, early in orders]
    awaited = [0, 1, 2, 3, 7, 6, 5, 4]
    positions = [
        jnp.minimum(lax.rem(intersection[b] - group + depth + groups, groups), block_count - 1)
        for b in range(block_count)
    ]
    loads[5].wait()
    for offset in offsets:
        answer(offset).wait_recv()
    for turn in range(min(len(offsets) // 2, rounds - 1), rounds):
        hear(turn)
    for target in order:
        block = jnp.zeros((rows, columns), jnp.float32)
        for b in range(block_count):
            block = block + jnp.dot(
                chosen[positions[b]],
                weights[b, :, pl.ds(pl.multiple_of(target * columns, columns), columns)],
                preferred_element_type=jnp.float32,
            )
        outbound[target] = block.astype(jnp.bfloat16)

        @pl.when(target == place)
        def _():
            arrived[target] = outbound[target]

        @pl.when(target != place)
        def _():
            deliver(target).start()

    def blend(origins, start, finish):
        for origin in origins:
            slab[origin] = arrived[origin].astype(jnp.float32)

        def mix(j, kept):
            first = j * TILE if isinstance(j, int) else pl.multiple_of(j * TILE, TILE)
            out_rows = pl.ds(first, TILE)
            kept_rows = pl.ds(first, kept)
            for piece in range(columns // 128):
                lanes = slice(piece * 128, (piece + 1) * 128)
                share = fraction[out_rows, lanes]
                rest = 1.0 - share
                below = [jnp.zeros((TILE, 128), jnp.float32)] * fields
                above = [jnp.zeros((TILE, 128), jnp.float32)] * fields
                for origin in origins:
                    lower = bracket[out_rows, lanes] - origin * level_slab
                    upper = lower + 1
                    lower_tile, upper_tile = lower >> 3, upper >> 3
                    lower_row, upper_row = lower & (TILE - 1), upper & (TILE - 1)
                    for tile in range(tiles):
                        in_lower, in_upper = lower_tile == tile, upper_tile == tile
                        for field in range(fields):
                            row = field * even + tile * TILE
                            values = slab[origin, row : row + TILE, lanes]
                            below[field] = jnp.where(in_lower, pick_rows(values, lower_row), below[field])
                            above[field] = jnp.where(in_upper, pick_rows(values, upper_row), above[field])
                    for extra in range(odd):
                        at_lower, at_upper = lower == even + extra, upper == even + extra
                        for field in range(fields):
                            row = full_rows + field * odd + extra
                            last = slab[origin, row : row + 1, lanes]
                            below[field] = jnp.where(at_lower, last, below[field])
                            above[field] = jnp.where(at_upper, last, above[field])
                for field in range(fields):
                    mixed = rest * below[field] + share * above[field]
                    if not start:
                        mixed = total[field, out_rows, lanes] + mixed
                    if finish:
                        out_ref[field, kept_rows, lanes] = mixed[0:kept].astype(jnp.bfloat16)
                    else:
                        total[field, out_rows, lanes] = mixed

        def step(j, carry):
            mix(j, TILE)
            return carry

        whole = levels_out // TILE
        lax.fori_loop(0, whole, step, 0)
        if levels_out % TILE:
            mix(whole, levels_out % TILE)

    turns = [awaited[0:3]] + [awaited[n : n + 2] for n in range(3, slabs, 2)]
    for n, origins in enumerate(turns):
        for origin in origins:

            @pl.when(origin != place)
            def _():
                await_slab(origin)

        blend(origins, n == 0, n == len(turns) - 1)

    for offset in offsets:
        ask(offset).wait_send()
        answer(offset).wait_send()
    for target in range(slabs):

        @pl.when(target != place)
        def _():
            deliver(target).wait_send()


def local(groups, slabs, source_state, intersection, index_map, blocks, bracket, fraction):
    fields, level_slab, tile_cells = source_state.shape
    block_count, width = index_map.shape
    levels_out, columns = bracket.shape
    out_rows = -(-levels_out // TILE) * TILE
    chunks = tile_cells // CHUNK
    rows = -(-fields * level_slab // TILE) * TILE
    rounds = slabs // 2 - 1
    any_spec = pl.BlockSpec(memory_space=pl.ANY)
    dma = pltpu.SemaphoreType.DMA

    return pl.pallas_call(
        functools.partial(kernel, groups, slabs),
        out_shape=pltpu.VMEM((fields, levels_out, columns), jnp.bfloat16),
        in_specs=[any_spec] * 6,
        out_specs=pl.BlockSpec(memory_space=pltpu.VMEM),
        scratch_shapes=[
            pltpu.VMEM(source_state.shape, jnp.bfloat16),
            pltpu.SMEM(intersection.shape, jnp.int32),
            pltpu.VMEM(index_map.shape, jnp.int32),
            pltpu.VMEM(blocks.shape, jnp.bfloat16),
            pltpu.VMEM(bracket.shape, jnp.int32),
            pltpu.VMEM(fraction.shape, jnp.float32),
            pltpu.VMEM((out_rows, columns), jnp.int32),
            pltpu.VMEM((out_rows, columns), jnp.float32),
            pltpu.VMEM((rows * chunks, CHUNK), jnp.bfloat16),
            pltpu.VMEM((block_count, 1, width), jnp.int32),
            pltpu.VMEM((block_count, 1, width), jnp.int32),
            pltpu.VMEM((block_count, rows, width), jnp.bfloat16),
            pltpu.VMEM((block_count, rows, width), jnp.bfloat16),
            pltpu.VMEM((slabs, rows, columns), jnp.bfloat16),
            pltpu.VMEM((slabs, rows, columns), jnp.bfloat16),
            pltpu.VMEM((slabs, rows, columns), jnp.float32),
            pltpu.VMEM((fields, out_rows, columns), jnp.float32),
            dma((6,)),
            dma((block_count,)),
            dma((block_count,)),
            dma((block_count,)),
            dma((block_count,)),
            dma((slabs,)),
            dma((slabs,)),
            pltpu.SemaphoreType.REGULAR((rounds,)),
            pltpu.SemaphoreType.REGULAR((rounds,)),
        ],
        compiler_params=pltpu.CompilerParams(
            collective_id=0, has_side_effects=True, vmem_limit_bytes=56 * 1024 * 1024
        ),
        name="regrid",
    )(source_state, intersection, index_map, blocks, bracket, fraction)


def solution(mesh):
    in_specs = (
        P(None, "lev", "horiz"),
        P("horiz"),
        P("horiz", None),
        P("horiz", None, None),
        P(None, ("horiz", "lev")),
        P(None, ("horiz", "lev")),
    )
    out_specs = P(None, None, ("horiz", "lev"))
    body = functools.partial(local, mesh.shape["horiz"], mesh.shape["lev"])
    return jax.shard_map(body, mesh=mesh, in_specs=in_specs, out_specs=out_specs, check_vma=False)
```

```python
import functools

import jax
import jax.numpy as jnp
from jax import lax
from jax.experimental import pallas as pl
from jax.experimental.pallas import tpu as pltpu
from jax.sharding import PartitionSpec as P

MESH = pl.DeviceIdType.MESH
CHUNK = 256
TILE = 8


def pick_rows(values, rows):
    return jnp.take_along_axis(values, rows, axis=0, mode="promise_in_bounds")


def kernel(
    groups,
    slabs,
    source_hbm,
    intersection_hbm,
    index_hbm,
    blocks_hbm,
    bracket_hbm,
    fraction_hbm,
    out_ref,
    source,
    intersection,
    index_map,
    weights,
    bracket_in,
    fraction_in,
    bracket,
    fraction,
    stacked,
    wanted,
    asked,
    picked,
    chosen,
    outbound,
    arrived,
    slab,
    total,
    local_sem,
    ask_send,
    ask_recv,
    value_send,
    value_recv,
    slab_send,
    slab_recv,
    rising,
    falling,
):
    group = lax.axis_index("horiz")
    place = lax.axis_index("lev")
    block_count = index_map.shape[0]
    depth = (block_count - 1) // 2
    fields, level_slab, tile_cells = source.shape
    chunks = tile_cells // CHUNK
    columns = bracket.shape[1]
    levels_out = bracket_in.shape[0]
    tiles = level_slab // TILE
    odd = level_slab - tiles * TILE
    even = tiles * TILE
    full_rows = fields * even
    rows = stacked.shape[0] // chunks
    offsets = list(range(1, depth + 1)) + list(range(-depth, 0))

    barrier = pltpu.get_barrier_semaphore()
    for offset in offsets:
        pl.semaphore_signal(
            barrier, inc=1, device_id={"horiz": lax.rem(group + offset + groups, groups)}, device_id_type=MESH
        )
    higher, lower_place = lax.rem(place + 1, slabs), lax.rem(place + slabs - 1, slabs)
    for neighbour in (higher, lower_place):
        pl.semaphore_signal(barrier, inc=1, device_id={"lev": neighbour}, device_id_type=MESH)

    loads = [
        pltpu.make_async_copy(src, dst, local_sem.at[n])
        for n, (src, dst) in enumerate(
            [
                (intersection_hbm, intersection),
                (index_hbm, index_map),
                (source_hbm, source),
                (bracket_hbm, bracket_in),
                (fraction_hbm, fraction_in),
                (blocks_hbm, weights),
            ]
        )
    ]
    for load in loads:
        load.start()
    loads[0].wait()
    loads[1].wait()

    for slot, offset in enumerate(range(-depth, depth + 1)):
        target = lax.rem(group + offset + groups, groups)
        row = jnp.zeros((1, index_map.shape[1]), jnp.int32)
        for block in range(block_count):
            row = row + jnp.where(intersection[block] == target, index_map[block : block + 1, :], 0)
        wanted[slot] = row

    pl.semaphore_wait(barrier, len(offsets) + 2)

    def ask(offset):
        slot = offset + depth
        return pltpu.make_async_remote_copy(
            src_ref=wanted.at[slot],
            dst_ref=asked.at[slot],
            send_sem=ask_send.at[slot],
            recv_sem=ask_recv.at[slot],
            device_id={"horiz": lax.rem(group + offset + groups, groups)},
            device_id_type=MESH,
        )

    def answer(offset):
        slot = offset + depth
        return pltpu.make_async_remote_copy(
            src_ref=picked.at[slot],
            dst_ref=chosen.at[slot],
            send_sem=value_send.at[slot],
            recv_sem=value_recv.at[slot],
            device_id={"horiz": lax.rem(group - offset + groups, groups)},
            device_id_type=MESH,
        )

    def deliver(target):
        return pltpu.make_async_remote_copy(
            src_ref=outbound.at[target],
            dst_ref=arrived.at[place],
            send_sem=slab_send.at[target],
            recv_sem=slab_recv.at[place],
            device_id={"lev": target},
            device_id_type=MESH,
        )

    def await_slab(origin):
        pltpu.make_async_remote_copy(
            src_ref=outbound.at[origin],
            dst_ref=arrived.at[origin],
            send_sem=slab_send.at[origin],
            recv_sem=slab_recv.at[origin],
            device_id={"lev": origin},
            device_id_type=MESH,
        ).wait_recv()

    rounds = slabs // 2 - 1

    def tell(turn):
        pl.semaphore_signal(rising.at[turn], inc=1, device_id={"lev": higher}, device_id_type=MESH)
        pl.semaphore_signal(falling.at[turn], inc=1, device_id={"lev": lower_place}, device_id_type=MESH)

    def hear(turn):
        pl.semaphore_wait(rising.at[turn], 1)
        pl.semaphore_wait(falling.at[turn], 1)
        if turn + 1 < rounds:
            tell(turn + 1)

    for offset in offsets:
        ask(offset).start()
    tell(0)

    loads[2].wait()
    for chunk in range(chunks):
        cells = slice(chunk * CHUNK, (chunk + 1) * CHUNK)
        base = chunk * rows
        for field in range(fields):
            stacked[base + field * even : base + (field + 1) * even, :] = source[field, 0:even, cells]
        last = [source[field, even:, cells].astype(jnp.float32) for field in range(fields)]
        last.append(jnp.zeros((rows - full_rows - fields * odd, CHUNK), jnp.float32))
        stacked[base + full_rows : base + rows, :] = jnp.concatenate(last, axis=0).astype(jnp.bfloat16)

    def select_cells(cell_ids, result_ref):
        for piece in range(cell_ids.shape[1] // CHUNK):
            cells = slice(piece * CHUNK, (piece + 1) * CHUNK)
            low = cell_ids[:, cells] & (CHUNK - 1)
            high = lax.shift_right_logical(cell_ids[:, cells], CHUNK.bit_length() - 1)
            picker = (
                (lax.broadcasted_iota(jnp.int32, (CHUNK, CHUNK), 0) == low).astype(jnp.float32).astype(jnp.bfloat16)
            )
            found = jnp.dot(stacked[...], picker, preferred_element_type=jnp.float32)
            result = jnp.zeros((rows, CHUNK), jnp.float32)
            for chunk in range(chunks):
                result = jnp.where(high == chunk, found[chunk * rows : (chunk + 1) * rows], result)
            result_ref[:, cells] = result.astype(jnp.bfloat16)

    select_cells(wanted[depth], chosen.at[depth])
    loads[3].wait()
    loads[4].wait()
    bracket[bracket.shape[0] - TILE :, :] = jnp.zeros((TILE, columns), jnp.int32)
    fraction[fraction.shape[0] - TILE :, :] = jnp.zeros((TILE, columns), jnp.float32)
    bracket[0:levels_out, :] = bracket_in[...]
    fraction[0:levels_out, :] = fraction_in[...]

    for turn, offset in enumerate(offsets):
        slot = offset + depth
        ask(offset).wait_recv()
        select_cells(asked[slot], picked.at[slot])
        answer(offset).start()
        if turn % 2 == 1 and turn // 2 < rounds - 1:
            hear(turn // 2)

    core = lax.rem(group, 2)
    orders = zip([1, 2, 0, 3, 7, 4, 6, 5], [0, 1, 7, 2, 6, 3, 5, 4])
    order = [early * core + late * (1 - core) for late, early in orders]
    awaited = [0, 1, 2, 3, 7, 6, 5, 4]
    positions = [
        jnp.minimum(lax.rem(intersection[b] - group + depth + groups, groups), block_count - 1)
        for b in range(block_count)
    ]
    loads[5].wait()
    for offset in offsets:
        answer(offset).wait_recv()
    for turn in range(min(len(offsets) // 2, rounds - 1), rounds):
        hear(turn)
    for target in order:
        block = jnp.zeros((rows, columns), jnp.float32)
        for b in range(block_count):
            block = block + jnp.dot(
                chosen[positions[b]],
                weights[b, :, pl.ds(pl.multiple_of(target * columns, columns), columns)],
                preferred_element_type=jnp.float32,
            )
        outbound[target] = block.astype(jnp.bfloat16)

        @pl.when(target == place)
        def _():
            arrived[target] = outbound[target]

        @pl.when(target != place)
        def _():
            deliver(target).start()

    def blend(origins, start, finish):
        for origin in origins:
            slab[origin] = arrived[origin].astype(jnp.float32)

        def mix(j, kept):
            first = j * TILE if isinstance(j, int) else pl.multiple_of(j * TILE, TILE)
            out_rows = pl.ds(first, TILE)
            kept_rows = pl.ds(first, kept)
            for piece in range(columns // 128):
                lanes = slice(piece * 128, (piece + 1) * 128)
                share = fraction[out_rows, lanes]
                rest = 1.0 - share
                below = [jnp.zeros((TILE, 128), jnp.float32)] * fields
                above = [jnp.zeros((TILE, 128), jnp.float32)] * fields
                for origin in origins:
                    lower = bracket[out_rows, lanes] - origin * level_slab
                    upper = lower + 1
                    lower_tile, upper_tile = lower >> 3, upper >> 3
                    lower_row, upper_row = lower & (TILE - 1), upper & (TILE - 1)
                    for tile in range(tiles):
                        in_lower, in_upper = lower_tile == tile, upper_tile == tile
                        for field in range(fields):
                            row = field * even + tile * TILE
                            values = slab[origin, row : row + TILE, lanes]
                            below[field] = jnp.where(in_lower, pick_rows(values, lower_row), below[field])
                            above[field] = jnp.where(in_upper, pick_rows(values, upper_row), above[field])
                    for extra in range(odd):
                        at_lower, at_upper = lower == even + extra, upper == even + extra
                        for field in range(fields):
                            row = full_rows + field * odd + extra
                            last = slab[origin, row : row + 1, lanes]
                            below[field] = jnp.where(at_lower, last, below[field])
                            above[field] = jnp.where(at_upper, last, above[field])
                for field in range(fields):
                    mixed = rest * below[field] + share * above[field]
                    if not start:
                        mixed = total[field, out_rows, lanes] + mixed
                    if finish:
                        out_ref[field, kept_rows, lanes] = mixed[0:kept].astype(jnp.bfloat16)
                    else:
                        total[field, out_rows, lanes] = mixed

        def step(j, carry):
            mix(j, TILE)
            return carry

        whole = levels_out // TILE
        lax.fori_loop(0, whole, step, 0, unroll=3)
        if levels_out % TILE:
            mix(whole, levels_out % TILE)

    turns = [awaited[0:3]] + [awaited[n : n + 2] for n in range(3, slabs, 2)]
    for n, origins in enumerate(turns):
        for origin in origins:

            @pl.when(origin != place)
            def _():
                await_slab(origin)

        blend(origins, n == 0, n == len(turns) - 1)

    for offset in offsets:
        ask(offset).wait_send()
        answer(offset).wait_send()
    for target in range(slabs):

        @pl.when(target != place)
        def _():
            deliver(target).wait_send()


def local(groups, slabs, source_state, intersection, index_map, blocks, bracket, fraction):
    fields, level_slab, tile_cells = source_state.shape
    block_count, width = index_map.shape
    levels_out, columns = bracket.shape
    out_rows = -(-levels_out // TILE) * TILE
    chunks = tile_cells // CHUNK
    rows = -(-fields * level_slab // TILE) * TILE
    rounds = slabs // 2 - 1
    any_spec = pl.BlockSpec(memory_space=pl.ANY)
    dma = pltpu.SemaphoreType.DMA

    return pl.pallas_call(
        functools.partial(kernel, groups, slabs),
        out_shape=pltpu.VMEM((fields, levels_out, columns), jnp.bfloat16),
        in_specs=[any_spec] * 6,
        out_specs=pl.BlockSpec(memory_space=pltpu.VMEM),
        scratch_shapes=[
            pltpu.VMEM(source_state.shape, jnp.bfloat16),
            pltpu.SMEM(intersection.shape, jnp.int32),
            pltpu.VMEM(index_map.shape, jnp.int32),
            pltpu.VMEM(blocks.shape, jnp.bfloat16),
            pltpu.VMEM(bracket.shape, jnp.int32),
            pltpu.VMEM(fraction.shape, jnp.float32),
            pltpu.VMEM((out_rows, columns), jnp.int32),
            pltpu.VMEM((out_rows, columns), jnp.float32),
            pltpu.VMEM((rows * chunks, CHUNK), jnp.bfloat16),
            pltpu.VMEM((block_count, 1, width), jnp.int32),
            pltpu.VMEM((block_count, 1, width), jnp.int32),
            pltpu.VMEM((block_count, rows, width), jnp.bfloat16),
            pltpu.VMEM((block_count, rows, width), jnp.bfloat16),
            pltpu.VMEM((slabs, rows, columns), jnp.bfloat16),
            pltpu.VMEM((slabs, rows, columns), jnp.bfloat16),
            pltpu.VMEM((slabs, rows, columns), jnp.float32),
            pltpu.VMEM((fields, out_rows, columns), jnp.float32),
            dma((6,)),
            dma((block_count,)),
            dma((block_count,)),
            dma((block_count,)),
            dma((block_count,)),
            dma((slabs,)),
            dma((slabs,)),
            pltpu.SemaphoreType.REGULAR((rounds,)),
            pltpu.SemaphoreType.REGULAR((rounds,)),
        ],
        compiler_params=pltpu.CompilerParams(
            collective_id=0, has_side_effects=True, vmem_limit_bytes=56 * 1024 * 1024
        ),
        name="regrid",
    )(source_state, intersection, index_map, blocks, bracket, fraction)


def solution(mesh):
    in_specs = (
        P(None, "lev", "horiz"),
        P("horiz"),
        P("horiz", None),
        P("horiz", None, None),
        P(None, ("horiz", "lev")),
        P(None, ("horiz", "lev")),
    )
    out_specs = P(None, None, ("horiz", "lev"))
    body = functools.partial(local, mesh.shape["horiz"], mesh.shape["lev"])
    return jax.shard_map(body, mesh=mesh, in_specs=in_specs, out_specs=out_specs, check_vma=False)
```

```python
import functools

import jax
import jax.numpy as jnp
from jax import lax
from jax.experimental import pallas as pl
from jax.experimental.pallas import tpu as pltpu
from jax.sharding import PartitionSpec as P

MESH = pl.DeviceIdType.MESH
CHUNK = 256
TILE = 8


def pick_rows(values, rows):
    return jnp.take_along_axis(values, rows, axis=0, mode="promise_in_bounds")


def kernel(
    groups,
    slabs,
    source_hbm,
    intersection_hbm,
    index_hbm,
    blocks_hbm,
    bracket_hbm,
    fraction_hbm,
    out_ref,
    source,
    intersection,
    index_map,
    weights,
    bracket_in,
    fraction_in,
    bracket,
    fraction,
    stacked,
    wanted,
    asked,
    picked,
    chosen,
    outbound,
    arrived,
    slab,
    total,
    partial,
    local_sem,
    ask_send,
    ask_recv,
    value_send,
    value_recv,
    slab_send,
    slab_recv,
    rising,
    falling,
):
    group = lax.axis_index("horiz")
    place = lax.axis_index("lev")
    block_count = index_map.shape[0]
    depth = (block_count - 1) // 2
    fields, level_slab, tile_cells = source.shape
    chunks = tile_cells // CHUNK
    columns = bracket.shape[1]
    levels_out = bracket_in.shape[0]
    tiles = level_slab // TILE
    odd = level_slab - tiles * TILE
    even = tiles * TILE
    full_rows = fields * even
    rows = stacked.shape[0] // chunks
    offsets = list(range(1, depth + 1)) + list(range(-depth, 0))

    barrier = pltpu.get_barrier_semaphore()
    for offset in offsets:
        pl.semaphore_signal(
            barrier, inc=1, device_id={"horiz": lax.rem(group + offset + groups, groups)}, device_id_type=MESH
        )
    higher, lower_place = lax.rem(place + 1, slabs), lax.rem(place + slabs - 1, slabs)
    for neighbour in (higher, lower_place):
        pl.semaphore_signal(barrier, inc=1, device_id={"lev": neighbour}, device_id_type=MESH)

    loads = [
        pltpu.make_async_copy(src, dst, local_sem.at[n])
        for n, (src, dst) in enumerate(
            [
                (intersection_hbm, intersection),
                (index_hbm, index_map),
                (source_hbm, source),
                (bracket_hbm, bracket_in),
                (fraction_hbm, fraction_in),
                (blocks_hbm, weights),
            ]
        )
    ]
    for load in loads:
        load.start()
    loads[0].wait()
    loads[1].wait()

    for slot, offset in enumerate(range(-depth, depth + 1)):
        target = lax.rem(group + offset + groups, groups)
        row = jnp.zeros((1, index_map.shape[1]), jnp.int32)
        for block in range(block_count):
            row = row + jnp.where(intersection[block] == target, index_map[block : block + 1, :], 0)
        wanted[slot] = row

    pl.semaphore_wait(barrier, len(offsets) + 2)

    def ask(offset):
        slot = offset + depth
        return pltpu.make_async_remote_copy(
            src_ref=wanted.at[slot],
            dst_ref=asked.at[slot],
            send_sem=ask_send.at[slot],
            recv_sem=ask_recv.at[slot],
            device_id={"horiz": lax.rem(group + offset + groups, groups)},
            device_id_type=MESH,
        )

    def answer(offset):
        slot = offset + depth
        return pltpu.make_async_remote_copy(
            src_ref=picked.at[slot],
            dst_ref=chosen.at[slot],
            send_sem=value_send.at[slot],
            recv_sem=value_recv.at[slot],
            device_id={"horiz": lax.rem(group - offset + groups, groups)},
            device_id_type=MESH,
        )

    def deliver(target):
        return pltpu.make_async_remote_copy(
            src_ref=outbound.at[target],
            dst_ref=arrived.at[place],
            send_sem=slab_send.at[target],
            recv_sem=slab_recv.at[place],
            device_id={"lev": target},
            device_id_type=MESH,
        )

    def await_slab(origin):
        pltpu.make_async_remote_copy(
            src_ref=outbound.at[origin],
            dst_ref=arrived.at[origin],
            send_sem=slab_send.at[origin],
            recv_sem=slab_recv.at[origin],
            device_id={"lev": origin},
            device_id_type=MESH,
        ).wait_recv()

    rounds = slabs // 2 - 1

    def tell(turn):
        pl.semaphore_signal(rising.at[turn], inc=1, device_id={"lev": higher}, device_id_type=MESH)
        pl.semaphore_signal(falling.at[turn], inc=1, device_id={"lev": lower_place}, device_id_type=MESH)

    def hear(turn):
        pl.semaphore_wait(rising.at[turn], 1)
        pl.semaphore_wait(falling.at[turn], 1)
        if turn + 1 < rounds:
            tell(turn + 1)

    for offset in offsets:
        ask(offset).start()
    tell(0)

    loads[2].wait()
    for chunk in range(chunks):
        cells = slice(chunk * CHUNK, (chunk + 1) * CHUNK)
        base = chunk * rows
        for field in range(fields):
            stacked[base + field * even : base + (field + 1) * even, :] = source[field, 0:even, cells]
        last = [source[field, even:, cells].astype(jnp.float32) for field in range(fields)]
        last.append(jnp.zeros((rows - full_rows - fields * odd, CHUNK), jnp.float32))
        stacked[base + full_rows : base + rows, :] = jnp.concatenate(last, axis=0).astype(jnp.bfloat16)

    def select_cells(cell_ids, result_ref):
        for piece in range(cell_ids.shape[1] // CHUNK):
            cells = slice(piece * CHUNK, (piece + 1) * CHUNK)
            low = cell_ids[:, cells] & (CHUNK - 1)
            high = lax.shift_right_logical(cell_ids[:, cells], CHUNK.bit_length() - 1)
            picker = (
                (lax.broadcasted_iota(jnp.int32, (CHUNK, CHUNK), 0) == low).astype(jnp.float32).astype(jnp.bfloat16)
            )
            found = jnp.dot(stacked[...], picker, preferred_element_type=jnp.float32)
            result = jnp.zeros((rows, CHUNK), jnp.float32)
            for chunk in range(chunks):
                result = jnp.where(high == chunk, found[chunk * rows : (chunk + 1) * rows], result)
            result_ref[:, cells] = result.astype(jnp.bfloat16)

    select_cells(wanted[depth], chosen.at[depth])
    loads[3].wait()
    loads[4].wait()
    bracket[bracket.shape[0] - TILE :, :] = jnp.zeros((TILE, columns), jnp.int32)
    fraction[fraction.shape[0] - TILE :, :] = jnp.zeros((TILE, columns), jnp.float32)
    bracket[0:levels_out, :] = bracket_in[...]
    fraction[0:levels_out, :] = fraction_in[...]

    for turn, offset in enumerate(offsets):
        slot = offset + depth
        ask(offset).wait_recv()
        select_cells(asked[slot], picked.at[slot])
        answer(offset).start()
        if turn % 2 == 1 and turn // 2 < rounds - 1:
            hear(turn // 2)

    core = lax.rem(group, 2)
    orders = zip([1, 2, 0, 3, 7, 4, 6, 5], [0, 1, 7, 2, 6, 3, 5, 4])
    order = [early * core + late * (1 - core) for late, early in orders]
    awaited = [0, 1, 2, 3, 7, 6, 5, 4]
    def block_of(offset):
        target = lax.rem(group + offset + groups, groups)
        number = jnp.int32(0)
        for b in range(block_count):
            number = number + jnp.where(intersection[b] == target, b, 0)
        return jnp.minimum(number, block_count - 1)

    def product(target, offset):
        return jnp.dot(
            chosen[offset + depth],
            weights[block_of(offset), :, pl.ds(pl.multiple_of(target * columns, columns), columns)],
            preferred_element_type=jnp.float32,
        )

    loads[5].wait()
    ready = offsets[:depth]
    for offset in ready:
        answer(offset).wait_recv()
    for target in order:
        partial[target] = sum([product(target, offset) for offset in ready], product(target, 0))
    for offset in offsets[depth:]:
        answer(offset).wait_recv()
    for turn in range(min(len(offsets) // 2, rounds - 1), rounds):
        hear(turn)
    for target in order:
        block = sum([product(target, offset) for offset in offsets[depth:]], partial[target])
        outbound[target] = block.astype(jnp.bfloat16)

        @pl.when(target == place)
        def _():
            arrived[target] = outbound[target]

        @pl.when(target != place)
        def _():
            deliver(target).start()

    def blend(origins, start, finish):
        for origin in origins:
            slab[origin] = arrived[origin].astype(jnp.float32)

        def mix(j, kept):
            first = j * TILE if isinstance(j, int) else pl.multiple_of(j * TILE, TILE)
            out_rows = pl.ds(first, TILE)
            kept_rows = pl.ds(first, kept)
            for piece in range(columns // 128):
                lanes = slice(piece * 128, (piece + 1) * 128)
                share = fraction[out_rows, lanes]
                rest = 1.0 - share
                below = [jnp.zeros((TILE, 128), jnp.float32)] * fields
                above = [jnp.zeros((TILE, 128), jnp.float32)] * fields
                for origin in origins:
                    lower = bracket[out_rows, lanes] - origin * level_slab
                    upper = lower + 1
                    lower_tile, upper_tile = lower >> 3, upper >> 3
                    lower_row, upper_row = lower & (TILE - 1), upper & (TILE - 1)
                    for tile in range(tiles):
                        in_lower, in_upper = lower_tile == tile, upper_tile == tile
                        for field in range(fields):
                            row = field * even + tile * TILE
                            values = slab[origin, row : row + TILE, lanes]
                            below[field] = jnp.where(in_lower, pick_rows(values, lower_row), below[field])
                            above[field] = jnp.where(in_upper, pick_rows(values, upper_row), above[field])
                    for extra in range(odd):
                        at_lower, at_upper = lower == even + extra, upper == even + extra
                        for field in range(fields):
                            row = full_rows + field * odd + extra
                            last = slab[origin, row : row + 1, lanes]
                            below[field] = jnp.where(at_lower, last, below[field])
                            above[field] = jnp.where(at_upper, last, above[field])
                for field in range(fields):
                    mixed = rest * below[field] + share * above[field]
                    if not start:
                        mixed = total[field, out_rows, lanes] + mixed
                    if finish:
                        out_ref[field, kept_rows, lanes] = mixed[0:kept].astype(jnp.bfloat16)
                    else:
                        total[field, out_rows, lanes] = mixed

        def step(j, carry):
            mix(j, TILE)
            return carry

        whole = levels_out // TILE
        lax.fori_loop(0, whole, step, 0, unroll=3)
        if levels_out % TILE:
            mix(whole, levels_out % TILE)

    turns = [awaited[0:3]] + [awaited[n : n + 2] for n in range(3, slabs, 2)]
    for n, origins in enumerate(turns):
        for origin in origins:

            @pl.when(origin != place)
            def _():
                await_slab(origin)

        blend(origins, n == 0, n == len(turns) - 1)

    for offset in offsets:
        ask(offset).wait_send()
        answer(offset).wait_send()
    for target in range(slabs):

        @pl.when(target != place)
        def _():
            deliver(target).wait_send()


def local(groups, slabs, source_state, intersection, index_map, blocks, bracket, fraction):
    fields, level_slab, tile_cells = source_state.shape
    block_count, width = index_map.shape
    levels_out, columns = bracket.shape
    out_rows = -(-levels_out // TILE) * TILE
    chunks = tile_cells // CHUNK
    rows = -(-fields * level_slab // TILE) * TILE
    rounds = slabs // 2 - 1
    any_spec = pl.BlockSpec(memory_space=pl.ANY)
    dma = pltpu.SemaphoreType.DMA

    return pl.pallas_call(
        functools.partial(kernel, groups, slabs),
        out_shape=pltpu.VMEM((fields, levels_out, columns), jnp.bfloat16),
        in_specs=[any_spec] * 6,
        out_specs=pl.BlockSpec(memory_space=pltpu.VMEM),
        scratch_shapes=[
            pltpu.VMEM(source_state.shape, jnp.bfloat16),
            pltpu.SMEM(intersection.shape, jnp.int32),
            pltpu.VMEM(index_map.shape, jnp.int32),
            pltpu.VMEM(blocks.shape, jnp.bfloat16),
            pltpu.VMEM(bracket.shape, jnp.int32),
            pltpu.VMEM(fraction.shape, jnp.float32),
            pltpu.VMEM((out_rows, columns), jnp.int32),
            pltpu.VMEM((out_rows, columns), jnp.float32),
            pltpu.VMEM((rows * chunks, CHUNK), jnp.bfloat16),
            pltpu.VMEM((block_count, 1, width), jnp.int32),
            pltpu.VMEM((block_count, 1, width), jnp.int32),
            pltpu.VMEM((block_count, rows, width), jnp.bfloat16),
            pltpu.VMEM((block_count, rows, width), jnp.bfloat16),
            pltpu.VMEM((slabs, rows, columns), jnp.bfloat16),
            pltpu.VMEM((slabs, rows, columns), jnp.bfloat16),
            pltpu.VMEM((slabs, rows, columns), jnp.float32),
            pltpu.VMEM((fields, out_rows, columns), jnp.float32),
            pltpu.VMEM((slabs, rows, columns), jnp.float32),
            dma((6,)),
            dma((block_count,)),
            dma((block_count,)),
            dma((block_count,)),
            dma((block_count,)),
            dma((slabs,)),
            dma((slabs,)),
            pltpu.SemaphoreType.REGULAR((rounds,)),
            pltpu.SemaphoreType.REGULAR((rounds,)),
        ],
        compiler_params=pltpu.CompilerParams(
            collective_id=0, has_side_effects=True, vmem_limit_bytes=56 * 1024 * 1024
        ),
        name="regrid",
    )(source_state, intersection, index_map, blocks, bracket, fraction)


def solution(mesh):
    in_specs = (
        P(None, "lev", "horiz"),
        P("horiz"),
        P("horiz", None),
        P("horiz", None, None),
        P(None, ("horiz", "lev")),
        P(None, ("horiz", "lev")),
    )
    out_specs = P(None, None, ("horiz", "lev"))
    body = functools.partial(local, mesh.shape["horiz"], mesh.shape["lev"])
    return jax.shard_map(body, mesh=mesh, in_specs=in_specs, out_specs=out_specs, check_vma=False)
```

```python
import functools

import jax
import jax.numpy as jnp
from jax import lax
from jax.experimental import pallas as pl
from jax.experimental.pallas import tpu as pltpu
from jax.sharding import PartitionSpec as P

MESH = pl.DeviceIdType.MESH
CHUNK = 256
TILE = 8


def pick_rows(values, rows):
    return jnp.take_along_axis(values, rows, axis=0, mode="promise_in_bounds")


def kernel(
    groups,
    slabs,
    source_hbm,
    intersection_hbm,
    index_hbm,
    blocks_hbm,
    bracket_hbm,
    fraction_hbm,
    out_ref,
    source,
    intersection,
    index_map,
    weights,
    bracket_in,
    fraction_in,
    bracket,
    fraction,
    stacked,
    wanted,
    asked,
    picked,
    chosen,
    outbound,
    arrived,
    slab,
    total,
    partial,
    local_sem,
    ask_send,
    ask_recv,
    value_send,
    value_recv,
    slab_send,
    slab_recv,
    rising,
    falling,
):
    group = lax.axis_index("horiz")
    place = lax.axis_index("lev")
    block_count = index_map.shape[0]
    depth = (block_count - 1) // 2
    fields, level_slab, tile_cells = source.shape
    chunks = tile_cells // CHUNK
    columns = bracket.shape[1]
    levels_out = bracket_in.shape[0]
    tiles = level_slab // TILE
    odd = level_slab - tiles * TILE
    even = tiles * TILE
    full_rows = fields * even
    rows = stacked.shape[0] // chunks
    offsets = list(range(1, depth + 1)) + list(range(-depth, 0))

    barrier = pltpu.get_barrier_semaphore()
    for offset in offsets:
        pl.semaphore_signal(
            barrier, inc=1, device_id={"horiz": lax.rem(group + offset + groups, groups)}, device_id_type=MESH
        )
    higher, lower_place = lax.rem(place + 1, slabs), lax.rem(place + slabs - 1, slabs)
    for neighbour in (higher, lower_place):
        pl.semaphore_signal(barrier, inc=1, device_id={"lev": neighbour}, device_id_type=MESH)

    loads = [
        pltpu.make_async_copy(src, dst, local_sem.at[n])
        for n, (src, dst) in enumerate(
            [
                (intersection_hbm, intersection),
                (index_hbm, index_map),
                (source_hbm, source),
                (bracket_hbm, bracket_in),
                (fraction_hbm, fraction_in),
                (blocks_hbm, weights),
            ]
        )
    ]
    for load in loads:
        load.start()
    loads[0].wait()
    loads[1].wait()

    for slot, offset in enumerate(range(-depth, depth + 1)):
        target = lax.rem(group + offset + groups, groups)
        row = jnp.zeros((1, index_map.shape[1]), jnp.int32)
        for block in range(block_count):
            row = row + jnp.where(intersection[block] == target, index_map[block : block + 1, :], 0)
        wanted[slot] = row

    pl.semaphore_wait(barrier, len(offsets) + 2)

    def ask(offset):
        slot = offset + depth
        return pltpu.make_async_remote_copy(
            src_ref=wanted.at[slot],
            dst_ref=asked.at[slot],
            send_sem=ask_send.at[slot],
            recv_sem=ask_recv.at[slot],
            device_id={"horiz": lax.rem(group + offset + groups, groups)},
            device_id_type=MESH,
        )

    def answer(offset):
        slot = offset + depth
        return pltpu.make_async_remote_copy(
            src_ref=picked.at[slot],
            dst_ref=chosen.at[slot],
            send_sem=value_send.at[slot],
            recv_sem=value_recv.at[slot],
            device_id={"horiz": lax.rem(group - offset + groups, groups)},
            device_id_type=MESH,
        )

    def deliver(target):
        return pltpu.make_async_remote_copy(
            src_ref=outbound.at[target],
            dst_ref=arrived.at[place],
            send_sem=slab_send.at[target],
            recv_sem=slab_recv.at[place],
            device_id={"lev": target},
            device_id_type=MESH,
        )

    def await_slab(origin):
        pltpu.make_async_remote_copy(
            src_ref=outbound.at[origin],
            dst_ref=arrived.at[origin],
            send_sem=slab_send.at[origin],
            recv_sem=slab_recv.at[origin],
            device_id={"lev": origin},
            device_id_type=MESH,
        ).wait_recv()

    rounds = slabs // 2 - 1

    def tell(turn):
        pl.semaphore_signal(rising.at[turn], inc=1, device_id={"lev": higher}, device_id_type=MESH)
        pl.semaphore_signal(falling.at[turn], inc=1, device_id={"lev": lower_place}, device_id_type=MESH)

    def hear(turn):
        pl.semaphore_wait(rising.at[turn], 1)
        pl.semaphore_wait(falling.at[turn], 1)
        if turn + 1 < rounds:
            tell(turn + 1)

    for offset in offsets:
        ask(offset).start()
    tell(0)

    loads[2].wait()
    for chunk in range(chunks):
        cells = slice(chunk * CHUNK, (chunk + 1) * CHUNK)
        base = chunk * rows
        for field in range(fields):
            stacked[base + field * even : base + (field + 1) * even, :] = source[field, 0:even, cells]
        last = [source[field, even:, cells].astype(jnp.float32) for field in range(fields)]
        last.append(jnp.zeros((rows - full_rows - fields * odd, CHUNK), jnp.float32))
        stacked[base + full_rows : base + rows, :] = jnp.concatenate(last, axis=0).astype(jnp.bfloat16)

    def select_cells(cell_ids, result_ref):
        for piece in range(cell_ids.shape[1] // CHUNK):
            cells = slice(piece * CHUNK, (piece + 1) * CHUNK)
            low = cell_ids[:, cells] & (CHUNK - 1)
            high = lax.shift_right_logical(cell_ids[:, cells], CHUNK.bit_length() - 1)
            picker = (
                (lax.broadcasted_iota(jnp.int32, (CHUNK, CHUNK), 0) == low).astype(jnp.float32).astype(jnp.bfloat16)
            )
            found = jnp.dot(stacked[...], picker, preferred_element_type=jnp.float32)
            result = jnp.zeros((rows, CHUNK), jnp.float32)
            for chunk in range(chunks):
                result = jnp.where(high == chunk, found[chunk * rows : (chunk + 1) * rows], result)
            result_ref[:, cells] = result.astype(jnp.bfloat16)

    select_cells(wanted[depth], chosen.at[depth])
    loads[3].wait()
    loads[4].wait()
    bracket[bracket.shape[0] - TILE :, :] = jnp.zeros((TILE, columns), jnp.int32)
    fraction[fraction.shape[0] - TILE :, :] = jnp.zeros((TILE, columns), jnp.float32)
    bracket[0:levels_out, :] = bracket_in[...]
    fraction[0:levels_out, :] = fraction_in[...]

    for turn, offset in enumerate(offsets):
        slot = offset + depth
        ask(offset).wait_recv()
        select_cells(asked[slot], picked.at[slot])
        answer(offset).start()
        if turn % 2 == 1 and turn // 2 < rounds - 1:
            hear(turn // 2)

    core = lax.rem(group, 2)
    orders = zip([1, 2, 0, 3, 7, 4, 6, 5], [0, 1, 7, 2, 6, 3, 5, 4])
    order = [early * core + late * (1 - core) for late, early in orders]
    awaited = [0, 1, 2, 3, 7, 6, 5, 4]
    def block_of(offset):
        target = lax.rem(group + offset + groups, groups)
        number = jnp.int32(0)
        for b in range(block_count):
            number = number + jnp.where(intersection[b] == target, b, 0)
        return jnp.minimum(number, block_count - 1)

    def product(target, offset):
        return jnp.dot(
            chosen[offset + depth],
            weights[block_of(offset), :, pl.ds(pl.multiple_of(target * columns, columns), columns)],
            preferred_element_type=jnp.float32,
        )

    loads[5].wait()
    ready = offsets[:depth]
    for offset in ready:
        answer(offset).wait_recv()
    for target in order:
        partial[target] = sum([product(target, offset) for offset in ready], product(target, 0))
    nearer, farther = core - 2, -1 - core
    answer(nearer).wait_recv()
    for target in order:
        partial[target] += product(target, nearer)
    answer(farther).wait_recv()
    for turn in range(min(len(offsets) // 2, rounds - 1), rounds):
        hear(turn)
    for target in order:
        block = partial[target] + product(target, farther)
        outbound[target] = block.astype(jnp.bfloat16)

        @pl.when(target == place)
        def _():
            arrived[target] = outbound[target]

        @pl.when(target != place)
        def _():
            deliver(target).start()

    def blend(origins, start, finish):
        for origin in origins:
            slab[origin] = arrived[origin].astype(jnp.float32)

        def mix(j, kept):
            first = j * TILE if isinstance(j, int) else pl.multiple_of(j * TILE, TILE)
            out_rows = pl.ds(first, TILE)
            kept_rows = pl.ds(first, kept)
            for piece in range(columns // 128):
                lanes = slice(piece * 128, (piece + 1) * 128)
                share = fraction[out_rows, lanes]
                rest = 1.0 - share
                below = [jnp.zeros((TILE, 128), jnp.float32)] * fields
                above = [jnp.zeros((TILE, 128), jnp.float32)] * fields
                for origin in origins:
                    lower = bracket[out_rows, lanes] - origin * level_slab
                    upper = lower + 1
                    lower_tile, upper_tile = lower >> 3, upper >> 3
                    lower_row, upper_row = lower & (TILE - 1), upper & (TILE - 1)
                    for tile in range(tiles):
                        in_lower, in_upper = lower_tile == tile, upper_tile == tile
                        for field in range(fields):
                            row = field * even + tile * TILE
                            values = slab[origin, row : row + TILE, lanes]
                            below[field] = jnp.where(in_lower, pick_rows(values, lower_row), below[field])
                            above[field] = jnp.where(in_upper, pick_rows(values, upper_row), above[field])
                    for extra in range(odd):
                        at_lower, at_upper = lower == even + extra, upper == even + extra
                        for field in range(fields):
                            row = full_rows + field * odd + extra
                            last = slab[origin, row : row + 1, lanes]
                            below[field] = jnp.where(at_lower, last, below[field])
                            above[field] = jnp.where(at_upper, last, above[field])
                for field in range(fields):
                    mixed = rest * below[field] + share * above[field]
                    if not start:
                        mixed = total[field, out_rows, lanes] + mixed
                    if finish:
                        out_ref[field, kept_rows, lanes] = mixed[0:kept].astype(jnp.bfloat16)
                    else:
                        total[field, out_rows, lanes] = mixed

        def step(j, carry):
            mix(j, TILE)
            return carry

        whole = levels_out // TILE
        lax.fori_loop(0, whole, step, 0, unroll=3)
        if levels_out % TILE:
            mix(whole, levels_out % TILE)

    turns = [awaited[0:3]] + [awaited[n : n + 2] for n in range(3, slabs, 2)]
    for n, origins in enumerate(turns):
        for origin in origins:

            @pl.when(origin != place)
            def _():
                await_slab(origin)

        blend(origins, n == 0, n == len(turns) - 1)

    for offset in offsets:
        ask(offset).wait_send()
        answer(offset).wait_send()
    for target in range(slabs):

        @pl.when(target != place)
        def _():
            deliver(target).wait_send()


def local(groups, slabs, source_state, intersection, index_map, blocks, bracket, fraction):
    fields, level_slab, tile_cells = source_state.shape
    block_count, width = index_map.shape
    levels_out, columns = bracket.shape
    out_rows = -(-levels_out // TILE) * TILE
    chunks = tile_cells // CHUNK
    rows = -(-fields * level_slab // TILE) * TILE
    rounds = slabs // 2 - 1
    any_spec = pl.BlockSpec(memory_space=pl.ANY)
    dma = pltpu.SemaphoreType.DMA

    return pl.pallas_call(
        functools.partial(kernel, groups, slabs),
        out_shape=pltpu.VMEM((fields, levels_out, columns), jnp.bfloat16),
        in_specs=[any_spec] * 6,
        out_specs=pl.BlockSpec(memory_space=pltpu.VMEM),
        scratch_shapes=[
            pltpu.VMEM(source_state.shape, jnp.bfloat16),
            pltpu.SMEM(intersection.shape, jnp.int32),
            pltpu.VMEM(index_map.shape, jnp.int32),
            pltpu.VMEM(blocks.shape, jnp.bfloat16),
            pltpu.VMEM(bracket.shape, jnp.int32),
            pltpu.VMEM(fraction.shape, jnp.float32),
            pltpu.VMEM((out_rows, columns), jnp.int32),
            pltpu.VMEM((out_rows, columns), jnp.float32),
            pltpu.VMEM((rows * chunks, CHUNK), jnp.bfloat16),
            pltpu.VMEM((block_count, 1, width), jnp.int32),
            pltpu.VMEM((block_count, 1, width), jnp.int32),
            pltpu.VMEM((block_count, rows, width), jnp.bfloat16),
            pltpu.VMEM((block_count, rows, width), jnp.bfloat16),
            pltpu.VMEM((slabs, rows, columns), jnp.bfloat16),
            pltpu.VMEM((slabs, rows, columns), jnp.bfloat16),
            pltpu.VMEM((slabs, rows, columns), jnp.float32),
            pltpu.VMEM((fields, out_rows, columns), jnp.float32),
            pltpu.VMEM((slabs, rows, columns), jnp.float32),
            dma((6,)),
            dma((block_count,)),
            dma((block_count,)),
            dma((block_count,)),
            dma((block_count,)),
            dma((slabs,)),
            dma((slabs,)),
            pltpu.SemaphoreType.REGULAR((rounds,)),
            pltpu.SemaphoreType.REGULAR((rounds,)),
        ],
        compiler_params=pltpu.CompilerParams(
            collective_id=0, has_side_effects=True, vmem_limit_bytes=56 * 1024 * 1024
        ),
        name="regrid",
    )(source_state, intersection, index_map, blocks, bracket, fraction)


def solution(mesh):
    in_specs = (
        P(None, "lev", "horiz"),
        P("horiz"),
        P("horiz", None),
        P("horiz", None, None),
        P(None, ("horiz", "lev")),
        P(None, ("horiz", "lev")),
    )
    out_specs = P(None, None, ("horiz", "lev"))
    body = functools.partial(local, mesh.shape["horiz"], mesh.shape["lev"])
    return jax.shard_map(body, mesh=mesh, in_specs=in_specs, out_specs=out_specs, check_vma=False)
```
